128 devices in a mesh: row: 2 (over core), col: 4 (over x), depth: 16 (over z, y).
Axes of the slice: x: 4, y: 4, z: 4, core: 2. Of those that a mesh axis runs over, the one named last changes fastest.
Arguments:
- normed: bfloat16 [512, 16, 4608], P('col', 'depth', 'row'), may hold values from -6 to 6
- qkv_grad: bfloat16 [512, 16, 8192], P('row', 'depth', 'col'), may hold values from -0.09375 to 0.09375
- attn_out: bfloat16 [512, 16, 4096], P('col', 'depth', 'row'), may hold values from -6 to 6
- out_grad: bfloat16 [512, 16, 4608], P('row', 'depth', 'col'), may hold values from -0.09375 to 0.09375
Outputs:
- qkv_weight_grad: float32 [4608, 8192], P('row', ('col', 'depth'))
- o_weight_grad: float32 [4096, 4608], P('row', ('col', 'depth'))
The draws below stay inside these ranges and needn't reach their ends.
All inputs are finite; a program needn't handle non-finite values.
Results may differ from the reference program's by a relative error of at most 0.0003.
Values may be sent and summed in bfloat16 or wider, within the bound.
A program may use at most 128 MiB of HBM per device.

```python
import jax
import jax.numpy as jnp
from jax import lax

D = 4608
QKV = 8192
HQW = 4096
TOK_DEPTH = 512
TOKENS = 8192
N_DEPTH = 16


def spiked(array, own_key, source, target, parts, factor):
    owner, partner = [(jnp.arange(array.shape[dim]) // (array.shape[dim] // parts)).reshape([-1 if axis == dim else 1 for axis in range(array.ndim)]) for dim in (source, target)]
    chosen = jax.random.permutation(own_key, parts)[partner]
    strong = (owner == chosen) | (owner == (partner + parts // 2) % parts)
    return jnp.where(strong, factor * array, array)


def block_levels(key, dims, pieces, smallest, top_value):
    loudness = 1.0
    for dim, blocks in pieces:
        draws = jax.random.uniform(jax.random.fold_in(jax.random.fold_in(key, 6), dim), (blocks,), jnp.float32, smallest / len(pieces), top_value / len(pieces))
        loudness = loudness * jnp.repeat(jnp.exp(draws), dims[dim] // blocks).reshape((-1,) + (1,) * (len(dims) - 1 - dim))
    return loudness


def centred(rng, shape, spread, reach, shards=(), kind=jnp.bfloat16):
    drawn = jax.random.normal(rng, shape, jnp.float32) * spread
    if len(shards) > 0:
        drawn = block_levels(rng, shape, shards, -0.22, 0.18) * drawn
    return jnp.clip(drawn, min=-reach, max=reach).astype(kind)


def noise_with(own_key, dims, scale, bound, split, heavy, kind=jnp.bfloat16):
    entries = scale * jax.random.normal(own_key, dims, jnp.float32)
    if split:
        entries = entries * block_levels(own_key, dims, split, -0.22, 0.18)
    return jnp.clip(spiked(entries, jax.random.fold_in(own_key, 3), *heavy), -bound, bound).astype(kind)


def setup_inputs(seed: int = 0) -> dict:
    key_list = jax.random.split(jax.random.key(seed), 5)
    normed = centred(key_list[0], (TOK_DEPTH, N_DEPTH, D), 1.0, 6.0, ((0, 4), (1, 16), (2, 2)))
    qkv_grad = noise_with(key_list[1], (TOK_DEPTH, N_DEPTH, QKV), (TOKENS ** -0.5), 0.09375, ((0, 2), (1, 16), (2, 4)), (1, 2, 16, 2.0))
    attn_out = centred(key_list[2], (TOK_DEPTH, N_DEPTH, HQW), 1.0, 6.0, ((0, 4), (1, 16), (2, 2)))
    out_grad = noise_with(key_list[3], (TOK_DEPTH, N_DEPTH, D), (TOKENS ** -0.5), 0.09375, ((0, 2), (1, 16), (2, 4)), (1, 2, 16, 2.0))
    return {"normed": normed, "qkv_grad": qkv_grad, "attn_out": attn_out, "out_grad": out_grad}


def outer_sum(left, right):
    return lax.dot_general(left, right, (((0, 1), (0, 1)), ((), ())), preferred_element_type=jnp.float32)


def reference(normed, qkv_grad, attn_out, out_grad):
    qkv_weight_grad = outer_sum(normed, qkv_grad)
    o_weight_grad = outer_sum(attn_out, out_grad)
    return (qkv_weight_grad, o_weight_grad)
```

```python
import functools

import jax
import jax.numpy as jnp
from jax import lax
from jax.experimental import pallas as pl
from jax.experimental.pallas import tpu as pltpu
from jax.sharding import PartitionSpec as P

MESH = pl.DeviceIdType.MESH
F32 = jnp.float32
BF16 = jnp.bfloat16

STEP = {1: 1, 2: -1, 3: 2}
N_SEM = 160


def kernel(
    a_q, b_q, a_o, b_o, out_q, out_o,
    sa_q, va_q, at_q, vb_q, c_q, r1_q, r2_q, f_q,
    sa_o, va_o, vb_o, bt_o, c_o, r1_o, r2_o, f_o,
    ssem, rsem, lsem, qsem,
):
    row, x, depth = lax.axis_index("row"), lax.axis_index("col"), lax.axis_index("depth")
    z, y = depth // 4, depth % 4

    def at(dx=0, dy=0, dz=0):
        return (row, (x + dx + 4) % 4, ((z + dz + 4) % 4) * 4 + (y + dy + 4) % 4)

    def on(axis, step):
        return at(**{"d" + axis: step})

    sibling = (1 - row, x, depth)

    count = {"r": 0, "l": 0}
    sent, kept = [], []

    def send(src, dst, device):
        k = count["r"]
        count["r"] += 1
        copy = pltpu.make_async_remote_copy(
            src, dst, ssem.at[k], rsem.at[k], device_id=device, device_id_type=MESH
        )
        copy.start()
        sent.append(copy)
        return copy

    def local(src, dst):
        k = count["l"]
        count["l"] += 1
        copy = pltpu.make_async_copy(src, dst, lsem.at[k])
        copy.start()
        return copy

    w_q, w_o = 512, 512
    loads_sa_q, loads_sa_o = [], []
    for d in (1, 2, 3):
        to = (z + STEP[d] + 4) % 4
        main = pl.ds(pl.multiple_of(to * w_q, 128), w_q)
        rest = pl.ds(pl.multiple_of(4 * w_q + (to // 2) * 128, 128), 128)
        loads_sa_q.append((
            local(a_q.at[:, main], sa_q.at[d - 1, :, 0:w_q]),
            local(a_q.at[:, rest], sa_q.at[d - 1, :, w_q:w_q + 128]),
        ))
    main = pl.ds(pl.multiple_of(z * w_q, 128), w_q)
    rest = pl.ds(pl.multiple_of(4 * w_q + (z // 2) * 128, 128), 128)
    load_va_q = (
        local(a_q.at[:, main], va_q.at[0, x, :, 0:w_q]),
        local(a_q.at[:, rest], va_q.at[0, x, :, w_q:w_q + 128]),
    )
    mine = pl.ds(pl.multiple_of(row * 256, 256), 256)
    load_vb_q = local(b_q, vb_q.at[0, mine, :])
    for d in (1, 2, 3):
        to = (y + STEP[d] + 4) % 4
        loads_sa_o.append(local(a_o.at[:, pl.ds(pl.multiple_of(to * w_o, 128), w_o)], sa_o.at[d - 1]))
    load_va_o = local(a_o.at[:, pl.ds(pl.multiple_of(y * w_o, 128), w_o)], va_o.at[0, x])
    load_vb_o = local(b_o, vb_o.at[0, mine, :])

    barrier = pltpu.get_barrier_semaphore()
    peers = [sibling, at(dx=1), at(dx=-1)]
    for axis in "yz":
        peers += [on(axis, 1), on(axis, -1), on(axis, 2)]
    for peer in peers:
        pl.semaphore_signal(barrier, inc=1, device_id=peer, device_id_type=MESH)
    pl.semaphore_wait(barrier, len(peers))

    ex_q, ex_o = {}, {}
    for d in (1, 2, 3):
        for copy in loads_sa_q[d - 1]:
            copy.wait()
        ex_q[d] = send(sa_q.at[d - 1], va_q.at[d, x], on("z", STEP[d]))
    for copy in load_va_q:
        copy.wait()
    gx_q, gx_o = {}, {}

    def spread(va, gx, s):
        gx[s, 1] = send(va.at[s, x], va.at[s, x], at(dx=1))
        gx[s, -1] = send(va.at[s, x], va.at[s, x], at(dx=-1))

    def pass_on(va, gx, s):
        step = 1 if s < 2 else -1
        gx[s, step].wait_recv()
        came = (x - step + 4) % 4
        gx[s, 2] = send(va.at[s, came], va.at[s, came], at(dx=step))

    def rest_of(gx, s):
        gx[s, -1 if s < 2 else 1].wait_recv()

    spread(va_q, gx_q, 0)
    for d in (1, 2, 3):
        loads_sa_o[d - 1].wait()
        ex_o[d] = send(sa_o.at[d - 1], va_o.at[d, x], on("y", STEP[d]))

    def b_direct(vb, axis, cols):
        src = vb.at[0, mine, cols]
        return (
            send(src, vb.at[1, mine, cols], on(axis, 1)),
            send(src, vb.at[2, mine, cols], on(axis, -1)),
        )

    halves = [pl.ds(pl.multiple_of(row * 256 + h * 128, 128), 128) for h in (0, 1)]

    def b_relay(vb, axis, cols, direct):
        across = []
        relay = []
        for d in (1, 2):
            direct[d - 1].wait_recv()
            part = vb.at[d, halves[d - 1], cols]
            relay.append(send(part, vb.at[3, halves[d - 1], cols], on(axis, STEP[d])))
            across.append(send(vb.at[d, mine, cols], vb.at[d, mine, cols], sibling))
        return relay, across

    def b_last(vb, cols, relay):
        across = []
        for d in (1, 2):
            relay[d - 1].wait_recv()
            part = vb.at[3, halves[d - 1], cols]
            across.append(send(part, part, sibling))
        return across

    cols_q = [slice(0, 1024), slice(1024, 2048)]
    all_o = slice(0, 1152)
    load_vb_q.wait()
    bd_q = [b_direct(vb_q, "z", cols_q[0])]
    own_q = send(vb_q.at[0, mine, :], vb_q.at[0, mine, :], sibling)
    load_vb_o.wait()
    bd_o = b_direct(vb_o, "y", all_o)
    own_o = send(vb_o.at[0, mine, :], vb_o.at[0, mine, :], sibling)
    load_va_o.wait()

    even = z % 2 == 0

    def turn_q(s, c):
        piece = va_q[s, c]
        k = s * 512 + c * 128
        at_q[0:512, pl.ds(pl.multiple_of(k, 128), 128)] = piece[:, 0:512].T
        tail = piece[:, 512:640].T
        at_q[512:576, pl.ds(pl.multiple_of(k, 128), 128)] = jnp.where(even, tail[0:64], tail[64:128])

    for d in (1, 2):
        ex_q[d].wait_recv()
        spread(va_q, gx_q, d)
    pass_on(va_q, gx_q, 0)
    ex_q[3].wait_recv()
    spread(va_q, gx_q, 3)
    for s in (1, 2, 3):
        pass_on(va_q, gx_q, s)

    spread(va_o, gx_o, 0)
    for d in (1, 2, 3):
        ex_o[d].wait_recv()
        spread(va_o, gx_o, d)

    relay_q0, across_q0 = b_relay(vb_q, "z", cols_q[0], bd_q[0])
    bd_q.append(b_direct(vb_q, "z", cols_q[1]))
    relay_o, across_o = b_relay(vb_o, "y", all_o, bd_o)

    for s in range(4):
        rest_of(gx_q, s)
        gx_q[s, 2].wait_recv()

        @pl.loop(0, 4)
        def _(c):
            turn_q(s, c)

    across_q0 += b_last(vb_q, cols_q[0], relay_q0)
    own_q.wait_recv()
    for copy in across_q0:
        copy.wait_recv()

    def multiply_q(j):
        @pl.loop(0, 2)
        def _(n):
            cols = pl.ds(pl.multiple_of(j * 512 + n * 256, 256), 256)
            right = vb_q[:, :, cols].reshape(2048, 256)
            total = jnp.dot(at_q[...], right, preferred_element_type=F32)
            for c in (0, 1):
                for h in (0, 1):
                    c_q[j, 2 * n + c, h] = total[h * 288:(h + 1) * 288, c * 128:(c + 1) * 128]

    def multiply_o():
        @pl.loop(0, 4)
        def _(w):
            for h in (0, 1):
                right = va_o[:, :, :, h * 256:(h + 1) * 256].reshape(2048, 256)
                total = jnp.dot(bt_o[w], right, preferred_element_type=F32)
                for j in range(4):
                    c_o[w, j, h] = total[j * 72:(j + 1) * 72]

    def sum_1(part, w, r1, r2, axis):
        return {
            1: send(part((w + 2) % 4, 0), r1.at[0], on(axis, 1)),
            2: send(part((w + 2) % 4, 1), r1.at[1], on(axis, -1)),
            3: send(part((w + 1) % 4, 1), r2.at[0, 1], on(axis, 1)),
            4: send(part((w + 3) % 4, 0), r2.at[1, 0], on(axis, -1)),
        }

    def sum_2(part, w, r1, r2, axis, go):
        go[1].wait_recv()
        ref = part((w + 1) % 4, 0)
        ref[...] = ref[...] + r1[0]
        go[5] = send(ref, r2.at[0, 0], on(axis, 1))
        go[2].wait_recv()
        ref = part((w + 3) % 4, 1)
        ref[...] = ref[...] + r1[1]
        go[6] = send(ref, r2.at[1, 1], on(axis, -1))

    def sum_3(part, w, r2, go, put):
        go[3].wait_recv()
        go[6].wait_recv()
        put(1, part(w, 1)[...] + r2[0, 1] + r2[1, 1])
        go[4].wait_recv()
        go[5].wait_recv()
        put(0, part(w, 0)[...] + r2[0, 0] + r2[1, 0])

    flip = ((z + 1) // 2) % 2
    order_q = [1 - flip, flip, 2 + flip, 3 - flip]
    parts_q = [lambda w, h, j=j: c_q.at[j, w, h] for j in order_q]
    go_q, go_o = {}, {}

    def q1(s):
        multiply_q(order_q[s])
        go_q[s] = sum_1(parts_q[s], y, r1_q.at[s], r2_q.at[s], "y")

    def q2(s):
        sum_2(parts_q[s], y, r1_q.at[s], r2_q.at[s], "y", go_q[s])

    rows_main = pl.ds(pl.multiple_of(z * 512, 512), 512)
    rows_rest = pl.ds(pl.multiple_of(2048 + z * 64, 64), 64)

    def home_q(s):
        j = order_q[s]
        delta = (j - z + 4) % 4
        device = (row, x, j * 4 + y)
        pair = []
        for i, (lo, n, rows) in enumerate(((0, 512, rows_main), (512, 64, rows_rest))):
            pair.append((
                pltpu.make_async_remote_copy(
                    f_q.at[s, lo:lo + n], out_q.at[rows], qsem.at[0, s, i], qsem.at[1, delta, i],
                    device_id=device, device_id_type=MESH,
                ),
                pltpu.make_async_copy(f_q.at[s, lo:lo + n], out_q.at[rows], qsem.at[0, s, i]),
            ))
        return delta, pair

    def q3(s):
        def put(h, value):
            f_q[s, h * 288:(h + 1) * 288] = value

        sum_3(parts_q[s], y, r2_q.at[s], go_q[s], put)
        delta, pair = home_q(s)

        @pl.when(delta != 0)
        def _():
            for far, near in pair:
                far.start()

        @pl.when(delta == 0)
        def _():
            for far, near in pair:
                near.start()

    order_o = [(y + 1 + s) % 4 for s in range(4)]
    parts_o = [lambda w, h, j=j: c_o.at[w, j, h] for j in order_o]

    def o1(s):
        go_o[s] = sum_1(parts_o[s], z, r1_o.at[s], r2_o.at[s], "z")

    def o2(s):
        sum_2(parts_o[s], z, r1_o.at[s], r2_o.at[s], "z", go_o[s])

    lanes_o = pl.ds(pl.multiple_of(y * 512, 512), 512)
    home_o = {}

    def o3(s):
        def put(h, value):
            f_o[s, :, h * 256:(h + 1) * 256] = value

        sum_3(parts_o[s], z, r2_o.at[s], go_o[s], put)
        if s < 3:
            home_o[s] = send(f_o.at[s], out_o.at[:, lanes_o], (row, x, z * 4 + order_o[s]))
        else:
            home_o[s] = local(f_o.at[s], out_o.at[:, lanes_o])

    def turn_o(s, r):
        bt_o[:, :, s * 512 + r * 256:s * 512 + (r + 1) * 256] = vb_o[s, r * 256:(r + 1) * 256].T.reshape(4, 288, 256)

    q1(0)
    pass_on(va_o, gx_o, 0)
    pass_on(va_o, gx_o, 1)
    q1(1)
    pass_on(va_o, gx_o, 2)
    pass_on(va_o, gx_o, 3)
    across_o += b_last(vb_o, all_o, relay_o)
    q2(0)
    own_o.wait_recv()
    for copy in across_o:
        copy.wait_recv()
    turn_o(0, 0)
    turn_o(0, 1)
    q2(1)
    turn_o(1, 0)
    turn_o(1, 1)
    relay_q1, across_q1 = b_relay(vb_q, "z", cols_q[1], bd_q[1])
    q3(0)
    turn_o(2, 0)
    turn_o(2, 1)
    turn_o(3, 0)
    turn_o(3, 1)
    for s in range(4):
        rest_of(gx_o, s)
        gx_o[s, 2].wait_recv()
    multiply_o()
    o1(0)
    o1(1)
    across_q1 += b_last(vb_q, cols_q[1], relay_q1)
    for copy in across_q1:
        copy.wait_recv()
    q1(2)
    q3(1)
    q1(3)
    o2(0)
    o1(2)
    o2(1)
    o1(3)
    q2(2)
    o3(0)
    o3(1)
    o2(2)
    o2(3)
    q2(3)
    o3(2)
    o3(3)
    q3(2)
    q3(3)

    for s in range(3):
        home_o[s].wait_recv()
    home_o[3].wait()
    for s in range(4):
        delta, pair = home_q(s)

        @pl.when(delta != 0)
        def _():
            for far, near in pair:
                far.wait_send()

        @pl.when(delta == 0)
        def _():
            for far, near in pair:
                near.wait()

    for d in (1, 2, 3):
        for i, (lo, n) in enumerate(((0, 512), (512, 64))):
            pltpu.make_async_remote_copy(
                f_q.at[0, lo:lo + n], out_q.at[lo:lo + n], qsem.at[0, 0, i], qsem.at[1, d, i],
                device_id=on("z", -d), device_id_type=MESH,
            ).wait_recv()
    for copy in sent:
        copy.wait_send()
    assert count["r"] <= N_SEM and count["l"] <= 24, count


def per_device(normed, qkv_grad, attn_out, out_grad):
    flat = [v.reshape(v.shape[0] * v.shape[1], v.shape[2]) for v in (normed, qkv_grad, attn_out, out_grad)]
    hbm = pl.BlockSpec(memory_space=pl.ANY)
    out_q, out_o = pl.pallas_call(
        kernel,
        out_shape=(
            jax.ShapeDtypeStruct((2304, 128), F32),
            jax.ShapeDtypeStruct((72, 2048), F32),
        ),
        in_specs=[hbm] * 4,
        out_specs=[hbm] * 2,
        scratch_shapes=[
            pltpu.VMEM((3, 128, 640), BF16),
            pltpu.VMEM((4, 4, 128, 640), BF16),
            pltpu.VMEM((576, 2048), BF16),
            pltpu.VMEM((4, 512, 2048), BF16),
            pltpu.VMEM((4, 4, 2, 288, 128), F32),
            pltpu.VMEM((4, 2, 288, 128), F32),
            pltpu.VMEM((4, 2, 2, 288, 128), F32),
            pltpu.VMEM((4, 576, 128), F32),
            pltpu.VMEM((3, 128, 512), BF16),
            pltpu.VMEM((4, 4, 128, 512), BF16),
            pltpu.VMEM((4, 512, 1152), BF16),
            pltpu.VMEM((4, 288, 2048), BF16),
            pltpu.VMEM((4, 4, 2, 72, 256), F32),
            pltpu.VMEM((4, 2, 72, 256), F32),
            pltpu.VMEM((4, 2, 2, 72, 256), F32),
            pltpu.VMEM((4, 72, 512), F32),
            pltpu.SemaphoreType.DMA((N_SEM,)),
            pltpu.SemaphoreType.DMA((N_SEM,)),
            pltpu.SemaphoreType.DMA((24,)),
            pltpu.SemaphoreType.DMA((2, 4, 2)),
        ],
        compiler_params=pltpu.CompilerParams(
            collective_id=0, has_side_effects=True, vmem_limit_bytes=60 * 1024 * 1024
        ),
        name="weight_grads",
    )(*flat)
    return out_q, out_o.T


def solution(mesh):
    in_specs = (
        P("col", "depth", "row"),
        P("row", "depth", "col"),
        P("col", "depth", "row"),
        P("row", "depth", "col"),
    )
    out_specs = (P("row", ("col", "depth")), P("row", ("col", "depth")))
    return jax.shard_map(
        per_device, mesh=mesh, in_specs=in_specs, out_specs=out_specs, check_vma=False
    )
```

```python
import jax
import jax.numpy as jnp
from jax import lax
from jax.experimental import pallas as pl
from jax.experimental.pallas import tpu as pltpu
from jax.sharding import PartitionSpec as P

MESH = pl.DeviceIdType.MESH
F32 = jnp.float32
BF16 = jnp.bfloat16

(EXQ, EXO, GQ, GO, HQ, HO, OWNQ, OWNO, DQ, DO, RQ, RO, AQ, AO, PQ, PO, IQ, IO, LQ, LO, FQ, FO) = range(22)
STEP = {1: 1, 2: -1, 3: 2}
N_SEM = 180


def kernel(
    a_q, b_q, a_o, b_o, out_q, out_o,
    la_q, ta_q, at_q, vb_q, c_q, r1_q, r2_q, f_q,
    sa_o, va_o, lb_o, bt_o, c_o, r1_o, r2_o, f_o,
    ssem, rsem, lsem,
):
    row, x, depth = lax.axis_index("row"), lax.axis_index("col"), lax.axis_index("depth")
    z, y = depth // 4, depth % 4

    def at(dx=0, dy=0, dz=0):
        return (row, (x + dx + 4) % 4, ((z + dz + 4) % 4) * 4 + (y + dy + 4) % 4)

    def on(axis, step):
        return at(**{"d" + axis: step})

    sibling = (1 - row, x, depth)

    barrier = pltpu.get_barrier_semaphore()
    peers = [sibling, at(dx=1), at(dx=-1)]
    for axis in "yz":
        peers += [on(axis, 1), on(axis, -1), on(axis, 2)]
    for peer in peers:
        pl.semaphore_signal(barrier, inc=1, device_id=peer, device_id_type=MESH)

    locals_ = []

    def local(src, dst):
        copy = pltpu.make_async_copy(src, dst, lsem.at[len(locals_)])
        copy.start()
        locals_.append(copy)
        return copy

    def lanes(start, size=128):
        return pl.ds(pl.multiple_of(start, 128), size)

    mine = lanes(row * 256, 256)
    load_la_q = local(a_q, la_q)
    load_lb_o = local(b_o, lb_o)
    loads = [local(b_q, vb_q.at[0, mine, :])]
    for d in (1, 2, 3):
        to = (y + STEP[d] + 4) % 4
        loads.append(local(a_o.at[:, lanes(to * 512, 512)], sa_o.at[d - 1]))
    loads.append(local(a_o.at[:, lanes(y * 512, 512)], va_o.at[0, x]))

    def features(u):
        return pl.ds(pl.multiple_of((u + 4) % 4 * 576, 64), 576)

    load_la_q.wait()
    ta_q[...] = la_q[...].T
    at_q[:, lanes(x * 128)] = ta_q[features(z), :]
    load_lb_o.wait()
    bt_o[:, :, lanes(row * 256, 256)] = lb_o[...].T.reshape(4, 288, 256)
    for copy in loads:
        copy.wait()
    pl.semaphore_wait(barrier, len(peers))

    flows = {}

    def flow(kind, number, which, *pieces):
        flows[kind, number, which] = pieces

    ahead, behind = (x + 1) % 4, (x + 3) % 4

    def piece_q(s, c):
        return at_q.at[:, lanes(s * 512 + c * 128)]

    for d in (1, 2, 3):
        flow(EXQ, d, 0, (ta_q.at[features(z + STEP[d]), :], piece_q(d, x), on("z", STEP[d])))
        flow(EXO, d, 0, (sa_o.at[d - 1], va_o.at[d, x], on("y", STEP[d])))
    for s in range(4):
        for step in (1, -1):
            src = ta_q.at[features(z), :] if s == 0 else piece_q(s, x)
            flow(GQ, s, step, (src, piece_q(s, x), at(dx=step)))
            flow(GO, s, step, (va_o.at[s, x], va_o.at[s, x], at(dx=step)))
            came_from = behind if step == 1 else ahead
            if s < 2:
                part_q, part_o = piece_q(s, came_from), va_o.at[s, came_from]
            else:
                half = slice(0, 288) if step == 1 else slice(288, 576)
                part_q = at_q.at[half, lanes(s * 512 + came_from * 128)]
                half = slice(0, 64) if step == 1 else slice(64, 128)
                part_o = va_o.at[s, came_from, half]
            flow(HQ, s, step, (part_q, part_q, at(dx=step)))
            flow(HO, s, step, (part_o, part_o, at(dx=step)))

    order_q = [(z + 1 + s) % 4 for s in range(4)]
    halves = [lanes(row * 256 + h * 128, 128) for h in (0, 1)]

    def strip(d, rows, j):
        return vb_q.at[d, rows, lanes((j + 4) % 4 * 512, 512)]

    def same(part, device):
        return (part, part, device)

    for p in range(4):
        flow(DQ, p, 1, (strip(0, mine, z + 2 + p), strip(1, mine, z + 2 + p), at(dz=1)))
        flow(DQ, p, -1, (strip(0, mine, z + p), strip(2, mine, z + p), at(dz=-1)))
        for d in (1, 2, 3):
            flow(AQ, p, d, same(strip(d, mine, order_q[p]), sibling))
        flow(AQ, p, 0, *[same(strip(d, mine, order_q[p]), sibling) for d in (1, 2, 3)])
    flow(RQ, 0, 0, (strip(1, mine, z + 2), strip(3, mine, z + 2), at(dz=1)))
    flow(RQ, 3, 1, (strip(1, halves[0], z + 1), strip(3, halves[0], z + 1), at(dz=1)))
    flow(RQ, 3, 2, (strip(1, halves[1], z + 1), strip(3, halves[1], z + 1), at(dz=1)))
    flow(RQ, 1, 0, (strip(2, mine, z + 1), strip(3, mine, z + 1), at(dz=-1)))
    flow(RQ, 2, 0, (strip(2, mine, z + 2), strip(3, mine, z + 2), at(dz=-1)))
    flow(OWNQ, 0, 0, same(vb_q.at[0, mine, :], sibling))

    def turned(d, p, first=0, size=256):
        return bt_o.at[2 * p:2 * p + 2, :, lanes(d * 512 + row * 256 + first, size)]

    for p in (0, 1):
        for d in (1, 2):
            flow(DO, p, STEP[d], (turned(0, p), turned(d, p), at(dy=STEP[d])))
            first = (d - 1) * 128
            flow(RO, p, STEP[d], (turned(d, p, first, 128), turned(3, p, first, 128), at(dy=STEP[d])))
        flow(AO, p, 0, same(turned(1, p), sibling), same(turned(2, p), sibling))
        flow(AO, p + 2, 0, same(turned(3, p), sibling))
    own = bt_o.at[:, :, lanes(row * 256, 256)]
    flow(OWNO, 0, 0, same(own, sibling))

    order_o = [(y + 1 + s) % 4 for s in range(4)]

    def part_q(s, w, h):
        return c_q.at[order_q[s], (w + 4) % 4, h]

    def part_o(s, w, h):
        return c_o.at[(w + 4) % 4, order_o[s], h]

    for s in range(4):
        for axis, w, part, r1, r2, (far, near, late) in (
            ("y", y, part_q, r1_q, r2_q, (PQ, IQ, LQ)),
            ("z", z, part_o, r1_o, r2_o, (PO, IO, LO)),
        ):
            up, down = on(axis, 1), on(axis, -1)
            flow(far, s, 1, (part(s, w + 2, 0), r1.at[s, 0], up))
            flow(far, s, -1, (part(s, w + 2, 1), r1.at[s, 1], down))
            flow(near, s, 1, (part(s, w + 1, 1), r2.at[s, 0, 1], up))
            flow(near, s, -1, (part(s, w - 1, 0), r2.at[s, 1, 0], down))
            flow(late, s, 1, (part(s, w + 1, 0), r2.at[s, 0, 0], up))
            flow(late, s, -1, (part(s, w - 1, 1), r2.at[s, 1, 1], down))
    home_q = out_q.at[features(z), :]
    home_o = out_o.at[:, lanes(y * 512, 512)]
    for s in range(3):
        flow(FQ, s, 0, (f_q.at[s], home_q, (row, x, order_q[s] * 4 + y)))
        flow(FO, s, 0, (f_o.at[s], home_o, (row, x, z * 4 + order_o[s])))

    def multiply_q(s):
        j = order_q[s]

        @pl.loop(0, 2)
        def _(n):
            right = vb_q[:, :, lanes(j * 512 + n * 256, 256)].reshape(2048, 256)
            total = jnp.dot(at_q[...], right, preferred_element_type=F32)
            for c in (0, 1):
                for h in (0, 1):
                    c_q[j, 2 * n + c, h] = total[h * 288:(h + 1) * 288, c * 128:(c + 1) * 128]

    def multiply_o(first):
        slots, k = (slice(0, 2), slice(0, 1024)) if first else (slice(2, 4), slice(1024, 2048))

        @pl.loop(0, 4)
        def _(w):
            for h in (0, 1):
                right = va_o[slots, :, :, h * 256:(h + 1) * 256].reshape(1024, 256)
                total = jnp.dot(bt_o[w, :, k], right, preferred_element_type=F32)
                for j in range(4):
                    part = total[j * 72:(j + 1) * 72]
                    c_o[w, j, h] = part if first else c_o[w, j, h] + part

    def join(s, w, part, r1):
        for ref, k in ((part(s, w + 1, 0), 0), (part(s, w - 1, 1), 1)):
            ref[...] = ref[...] + r1[s, k]

    def join_q(s):
        join(s, y, part_q, r1_q)

    def join_o(s):
        join(s, z, part_o, r1_o)

    def finish_q(s):
        for h in (0, 1):
            rows = slice(h * 288, (h + 1) * 288)
            total = part_q(s, y, h)[...] + r2_q[s, 0, h] + r2_q[s, 1, h]
            if s < 3:
                f_q[s, rows] = total
            else:
                out_q[pl.ds(pl.multiple_of(z * 576 + h * 288, 32), 288)] = total

    def finish_o(s):
        for h in (0, 1):
            total = part_o(s, z, h)[...] + r2_o[s, 0, h] + r2_o[s, 1, h]
            if s < 3:
                f_o[s, :, h * 256:(h + 1) * 256] = total
            else:
                out_o[:, lanes(y * 512 + h * 256, 256)] = total

    copies, n_sent = {}, [0]
    open_left, open_came = {}, {}

    def send(*names):
        for name in names:
            copies[name] = []
            for src, dst, device in flows[name]:
                k = n_sent[0]
                n_sent[0] += 1
                copy = pltpu.make_async_remote_copy(
                    src, dst, ssem.at[k], rsem.at[k], device_id=device, device_id_type=MESH
                )
                copy.start()
                copies[name].append(copy)
            open_left[name] = open_came[name] = True

    def left(*names):
        for name in names:
            del open_left[name]
            for copy in copies[name]:
                copy.wait_send()

    def came(*names):
        for name in names:
            del open_came[name]
            for copy in copies[name]:
                copy.wait_recv()

    send((EXO, 1, 0), (EXO, 2, 0))
    send((EXQ, 1, 0), (EXQ, 2, 0))
    send((GQ, 0, 1), (GQ, 0, -1))
    left((EXO, 1, 0), (EXO, 2, 0))
    send((EXO, 3, 0))
    send((EXQ, 3, 0))
    came((EXQ, 2, 0))
    send((GQ, 2, 1), (GQ, 2, -1))
    send((OWNQ, 0, 0), (OWNO, 0, 0))
    left((EXQ, 1, 0), (EXQ, 2, 0))
    send((DQ, 0, 1), (DQ, 0, -1))
    left((EXO, 3, 0))
    send((DO, 0, 1), (DO, 0, -1))
    left((GQ, 0, 1))
    came((EXQ, 1, 0))
    send((GQ, 1, 1), (GQ, 1, -1))
    came((EXQ, 3, 0))
    send((GQ, 3, 1), (GQ, 3, -1))
    left((DQ, 0, 1))
    send((DQ, 1, 1))
    left((GQ, 1, 1))
    came((GQ, 0, 1))
    send((HQ, 0, 1))
    left((DO, 0, 1), (DO, 0, -1))
    send((DO, 1, 1), (DO, 1, -1))
    left((GQ, 1, -1))
    came((GQ, 1, -1))
    send((HQ, 1, -1))
    left((DQ, 0, -1))
    send((DQ, 1, -1))
    left((HQ, 0, 1))
    came((GQ, 2, 1), (GQ, 2, -1))
    send((HQ, 2, 1), (HQ, 2, -1))
    came((DQ, 0, -1), (DQ, 0, 1))
    send((AQ, 0, 1), (AQ, 0, 2))
    send((RQ, 1, 0))
    came((EXO, 3, 0))
    send((GO, 3, 1), (GO, 3, -1))
    came((DQ, 1, 1))
    send((RQ, 0, 0), (AQ, 1, 1))
    came((EXO, 1, 0))
    send((GO, 1, 1), (GO, 1, -1))
    came((GQ, 3, 1), (GQ, 3, -1))
    send((HQ, 3, 1), (HQ, 3, -1))
    came((DO, 0, 1), (DO, 0, -1))
    send((RO, 0, 1), (RO, 0, -1), (AO, 0, 0))
    came((DO, 1, 1), (DO, 1, -1))
    send((RO, 1, 1), (RO, 1, -1), (AO, 1, 0))
    left((RQ, 0, 0))
    send((DQ, 2, 1))
    send((GO, 0, 1), (GO, 0, -1))
    left((DQ, 1, -1), (RQ, 1, 0))
    send((DQ, 2, -1))
    came((RQ, 0, 0))
    send((AQ, 0, 3))
    came((RO, 1, 1), (RO, 1, -1))
    send((AO, 3, 0))
    send((RQ, 3, 2))
    came((DQ, 1, -1))
    send((AQ, 1, 2))
    send((RQ, 2, 0))
    came((RQ, 1, 0))
    send((AQ, 1, 3))
    came((EXO, 2, 0))
    send((GO, 2, 1), (GO, 2, -1))
    came((GO, 3, 1), (GO, 3, -1))
    send((HO, 3, 1), (HO, 3, -1))
    came((GQ, 0, -1), (HQ, 0, 1), (GQ, 1, 1), (HQ, 1, -1), (HQ, 2, 1), (HQ, 2, -1), (HQ, 3, 1), (HQ, 3, -1))
    came((AQ, 0, 1), (AQ, 0, 2), (AQ, 0, 3), (OWNQ, 0, 0))
    multiply_q(0)
    send((PQ, 0, 1), (PQ, 0, -1))
    came((GO, 1, -1))
    send((HO, 1, -1))
    left((DQ, 1, 1))
    send((RQ, 3, 1))
    came((RO, 0, 1), (RO, 0, -1))
    send((AO, 2, 0))
    came((AQ, 1, 1), (AQ, 1, 2), (AQ, 1, 3))
    multiply_q(1)
    send((PQ, 1, 1), (PQ, 1, -1))
    left((GO, 1, 1))
    came((GO, 0, 1))
    send((HO, 0, 1))
    left((DQ, 2, -1))
    send((DQ, 3, -1))
    send((IQ, 0, 1), (IQ, 0, -1))
    left((DQ, 2, 1), (RQ, 3, 2))
    send((DQ, 3, 1))
    send((IQ, 1, 1), (IQ, 1, -1))
    came((GO, 2, 1), (GO, 2, -1))
    send((HO, 2, 1), (HO, 2, -1))
    came((OWNO, 0, 0), (AO, 0, 0), (AO, 1, 0), (AO, 2, 0), (AO, 3, 0), (GO, 0, -1), (HO, 0, 1), (GO, 1, 1))
    came((HO, 1, -1))
    multiply_o(True)
    came((PQ, 0, 1), (PQ, 0, -1))
    join_q(0)
    send((LQ, 0, 1), (LQ, 0, -1))
    came((HO, 2, 1), (HO, 2, -1), (HO, 3, 1), (HO, 3, -1))
    multiply_o(False)
    send((PO, 3, 1), (PO, 3, -1), (IO, 3, 1), (IO, 3, -1))
    came((DQ, 2, 1), (DQ, 2, -1), (RQ, 2, 0))
    send((AQ, 2, 0))
    came((DQ, 3, 1), (DQ, 3, -1), (RQ, 3, 1), (RQ, 3, 2))
    send((AQ, 3, 0))
    send((PO, 2, 1), (PO, 2, -1), (IO, 2, 1), (IO, 2, -1))
    send((PO, 0, 1), (PO, 0, -1), (IO, 0, 1), (IO, 0, -1))
    came((PQ, 1, 1), (PQ, 1, -1))
    join_q(1)
    send((LQ, 1, 1), (LQ, 1, -1))
    came((AQ, 2, 0))
    multiply_q(2)
    send((PQ, 2, 1), (PQ, 2, -1))
    came((PO, 3, 1), (PO, 3, -1))
    join_o(3)
    send((LO, 3, 1), (LO, 3, -1))
    send((IQ, 2, 1), (IQ, 2, -1))
    came((IQ, 1, 1), (IQ, 1, -1), (LQ, 1, 1), (LQ, 1, -1))
    finish_q(1)
    send((FQ, 1, 0))
    came((AQ, 3, 0))
    multiply_q(3)
    send((PQ, 3, 1), (PQ, 3, -1))
    left((PO, 0, 1))
    send((PO, 1, 1), (PO, 1, -1), (IO, 1, 1), (IO, 1, -1))
    came((IO, 3, 1), (IO, 3, -1), (LO, 3, 1), (LO, 3, -1))
    finish_o(3)
    came((PQ, 2, 1), (PQ, 2, -1))
    join_q(2)
    send((LQ, 2, 1), (LQ, 2, -1))
    came((PO, 0, 1), (PO, 0, -1))
    join_o(0)
    send((LO, 0, 1), (LO, 0, -1))
    left((PQ, 3, 1))
    send((IQ, 3, 1), (IQ, 3, -1))
    came((PO, 2, 1), (PO, 2, -1))
    join_o(2)
    send((LO, 2, 1), (LO, 2, -1))
    came((PO, 1, 1), (PO, 1, -1))
    join_o(1)
    send((LO, 1, 1), (LO, 1, -1))
    came((PQ, 3, 1), (PQ, 3, -1))
    join_q(3)
    send((LQ, 3, 1), (LQ, 3, -1))
    came((IQ, 2, 1), (IQ, 2, -1), (LQ, 2, 1), (LQ, 2, -1))
    finish_q(2)
    send((FQ, 2, 0))
    came((IQ, 0, 1), (IQ, 0, -1), (LQ, 0, 1), (LQ, 0, -1))
    finish_q(0)
    send((FQ, 0, 0))
    came((IO, 2, 1), (IO, 2, -1), (LO, 2, 1), (LO, 2, -1))
    finish_o(2)
    send((FO, 2, 0))
    came((IO, 0, 1), (IO, 0, -1), (LO, 0, 1), (LO, 0, -1))
    finish_o(0)
    send((FO, 0, 0))
    came((IQ, 3, 1), (IQ, 3, -1), (LQ, 3, 1), (LQ, 3, -1))
    finish_q(3)
    came((IO, 1, 1), (IO, 1, -1), (LO, 1, 1), (LO, 1, -1))
    finish_o(1)
    send((FO, 1, 0))

    came(*list(open_came))
    left(*list(open_left))
    assert n_sent[0] <= N_SEM and len(locals_) == 7, (n_sent, len(locals_))


def per_device(normed, qkv_grad, attn_out, out_grad):
    flat = [v.reshape(v.shape[0] * v.shape[1], v.shape[2]) for v in (normed, qkv_grad, attn_out, out_grad)]
    hbm = pl.BlockSpec(memory_space=pltpu.HBM)
    vmem = pl.BlockSpec(memory_space=pltpu.VMEM)
    out_q, out_o = pl.pallas_call(
        kernel,
        out_shape=(
            jax.ShapeDtypeStruct((2304, 128), F32),
            jax.ShapeDtypeStruct((72, 2048), F32),
        ),
        in_specs=[hbm] * 4,
        out_specs=[vmem] * 2,
        scratch_shapes=[
            pltpu.VMEM((128, 2304), BF16),
            pltpu.VMEM((2304, 128), BF16),
            pltpu.VMEM((576, 2048), BF16),
            pltpu.VMEM((4, 512, 2048), BF16),
            pltpu.VMEM((4, 4, 2, 288, 128), F32),
            pltpu.VMEM((4, 2, 288, 128), F32),
            pltpu.VMEM((4, 2, 2, 288, 128), F32),
            pltpu.VMEM((3, 576, 128), F32),
            pltpu.VMEM((3, 128, 512), BF16),
            pltpu.VMEM((4, 4, 128, 512), BF16),
            pltpu.VMEM((256, 1152), BF16),
            pltpu.VMEM((4, 288, 2048), BF16),
            pltpu.VMEM((4, 4, 2, 72, 256), F32),
            pltpu.VMEM((4, 2, 72, 256), F32),
            pltpu.VMEM((4, 2, 2, 72, 256), F32),
            pltpu.VMEM((3, 72, 512), F32),
            pltpu.SemaphoreType.DMA((N_SEM,)),
            pltpu.SemaphoreType.DMA((N_SEM,)),
            pltpu.SemaphoreType.DMA((7,)),
        ],
        compiler_params=pltpu.CompilerParams(
            collective_id=0, has_side_effects=True, vmem_limit_bytes=40 * 1024 * 1024
        ),
        name="weight_grads",
    )(*[pltpu.with_memory_space_constraint(v, pltpu.HBM) for v in flat])
    return out_q, out_o.T


def solution(mesh):
    in_specs = (
        P("col", "depth", "row"),
        P("row", "depth", "col"),
        P("col", "depth", "row"),
        P("row", "depth", "col"),
    )
    out_specs = (P("row", ("col", "depth")), P("row", ("col", "depth")))
    return jax.shard_map(
        per_device, mesh=mesh, in_specs=in_specs, out_specs=out_specs, check_vma=False
    )
```

```python
import jax
import jax.numpy as jnp
from jax import lax
from jax.experimental import pallas as pl
from jax.experimental.pallas import tpu as pltpu
from jax.sharding import PartitionSpec as P

MESH = pl.DeviceIdType.MESH
F32 = jnp.float32
BF16 = jnp.bfloat16

(EXQ, EXO, GQ, GO, HQ, HO, OWNQ, OWNO, DQ, DO, RQ, RO, AQ, AO, PQ, PO, IQ, IO, LQ, LO, FQ, FO) = range(22)
STEP = {1: 1, 2: -1, 3: 2}
N_SEND, N_COME = 27, 96


def kernel(
    a_q, b_q, a_o, b_o, out_q, out_o,
    la_q, ta_q, at_q, vb_q, c_q, r1_q, r2_q, f_q,
    sa_o, va_o, lb_o, bt_o, c_o, r1_o, r2_o, f_o,
    ssem, rsem, lsem,
):
    row, x, depth = lax.axis_index("row"), lax.axis_index("col"), lax.axis_index("depth")
    z, y = depth // 4, depth % 4

    def at(dx=0, dy=0, dz=0):
        return (row, (x + dx + 4) % 4, ((z + dz + 4) % 4) * 4 + (y + dy + 4) % 4)

    def on(axis, step):
        return at(**{"d" + axis: step})

    sibling = (1 - row, x, depth)

    barrier = pltpu.get_barrier_semaphore()
    peers = [sibling, at(dx=1), at(dx=-1)]
    for axis in "yz":
        peers += [on(axis, 1), on(axis, -1), on(axis, 2)]
    for peer in peers:
        pl.semaphore_signal(barrier, inc=1, device_id=peer, device_id_type=MESH)

    locals_ = []

    def local(src, dst):
        copy = pltpu.make_async_copy(src, dst, lsem.at[len(locals_)])
        copy.start()
        locals_.append(copy)
        return copy

    def lanes(start, size=128):
        return pl.ds(pl.multiple_of(start, 128), size)

    mine = lanes(row * 256, 256)
    load_la_q = local(a_q, la_q)
    load_lb_o = local(b_o, lb_o)
    loads = [local(b_q, vb_q.at[0, mine, :])]
    for d in (1, 2, 3):
        to = (y + STEP[d] + 4) % 4
        loads.append(local(a_o.at[:, lanes(to * 512, 512)], sa_o.at[d - 1]))
    loads.append(local(a_o.at[:, lanes(y * 512, 512)], va_o.at[0, x]))

    def features(u):
        return pl.ds(pl.multiple_of((u + 4) % 4 * 576, 64), 576)

    load_la_q.wait()
    ta_q[...] = la_q[...].T
    at_q[:, lanes(x * 128)] = ta_q[features(z), :]
    load_lb_o.wait()
    bt_o[:, :, lanes(row * 256, 256)] = lb_o[...].T.reshape(4, 288, 256)
    for copy in loads:
        copy.wait()
    pl.semaphore_wait(barrier, len(peers))

    flows = {}

    def flow(kind, number, which, *pieces):
        flows[kind, number, which] = pieces

    ahead, behind = (x + 1) % 4, (x + 3) % 4

    def piece_q(s, c):
        return at_q.at[:, lanes(s * 512 + c * 128)]

    for d in (1, 2, 3):
        flow(EXQ, d, 0, (ta_q.at[features(z + STEP[d]), :], piece_q(d, x), on("z", STEP[d])))
        flow(EXO, d, 0, (sa_o.at[d - 1], va_o.at[d, x], on("y", STEP[d])))
    for s in range(4):
        for step in (1, -1):
            src = ta_q.at[features(z), :] if s == 0 else piece_q(s, x)
            flow(GQ, s, step, (src, piece_q(s, x), at(dx=step)))
            flow(GO, s, step, (va_o.at[s, x], va_o.at[s, x], at(dx=step)))
            came_from = behind if step == 1 else ahead
            if s < 2:
                part_q, part_o = piece_q(s, came_from), va_o.at[s, came_from]
            else:
                half = slice(0, 288) if step == 1 else slice(288, 576)
                part_q = at_q.at[half, lanes(s * 512 + came_from * 128)]
                half = slice(0, 64) if step == 1 else slice(64, 128)
                part_o = va_o.at[s, came_from, half]
            flow(HQ, s, step, (part_q, part_q, at(dx=step)))
            flow(HO, s, step, (part_o, part_o, at(dx=step)))

    order_q = [(z + 1 + s) % 4 for s in range(4)]
    halves = [lanes(row * 256 + h * 128, 128) for h in (0, 1)]

    def strip(d, rows, j):
        return vb_q.at[d, rows, lanes((j + 4) % 4 * 512, 512)]

    def same(part, device):
        return (part, part, device)

    for p in range(4):
        flow(DQ, p, 1, (strip(0, mine, z + 2 + p), strip(1, mine, z + 2 + p), at(dz=1)))
        flow(DQ, p, -1, (strip(0, mine, z + p), strip(2, mine, z + p), at(dz=-1)))
        for d in (1, 2, 3):
            flow(AQ, p, d, same(strip(d, mine, order_q[p]), sibling))
        flow(AQ, p, 0, *[same(strip(d, mine, order_q[p]), sibling) for d in (1, 2, 3)])
    for h in (0, 1):
        flow(DQ, 1, h + 2, (strip(0, halves[h], z + 3), strip(1, halves[h], z + 3), at(dz=1)))
        flow(RQ, 0, h, (strip(1, halves[h], z + 2), strip(3, halves[h], z + 2), at(dz=1)))
        flow(AQ, 0, h + 4, same(strip(3, halves[h], order_q[0]), sibling))
    flow(RQ, 3, 1, (strip(1, halves[0], z + 1), strip(3, halves[0], z + 1), at(dz=1)))
    flow(RQ, 3, 2, (strip(1, halves[1], z + 1), strip(3, halves[1], z + 1), at(dz=1)))
    flow(RQ, 1, 0, (strip(2, mine, z + 1), strip(3, mine, z + 1), at(dz=-1)))
    flow(RQ, 2, 0, (strip(2, mine, z + 2), strip(3, mine, z + 2), at(dz=-1)))
    flow(OWNQ, 0, 0, same(vb_q.at[0, mine, :], sibling))

    def turned(d, p, first=0, size=256):
        return bt_o.at[2 * p:2 * p + 2, :, lanes(d * 512 + row * 256 + first, size)]

    for p in (0, 1):
        for d in (1, 2):
            flow(DO, p, STEP[d], (turned(0, p), turned(d, p), at(dy=STEP[d])))
            first = (d - 1) * 128
            flow(RO, p, STEP[d], (turned(d, p, first, 128), turned(3, p, first, 128), at(dy=STEP[d])))
        flow(AO, p, 0, same(turned(1, p), sibling), same(turned(2, p), sibling))
        flow(AO, p + 2, 0, same(turned(3, p), sibling))
    own = bt_o.at[:, :, lanes(row * 256, 256)]
    flow(OWNO, 0, 0, same(own, sibling))

    order_o = [(y + 1 + s) % 4 for s in range(4)]

    def part_q(s, w, h):
        return c_q.at[order_q[s], (w + 4) % 4, h]

    def part_o(s, w, h):
        return c_o.at[(w + 4) % 4, order_o[s], h]

    for s in range(4):
        for axis, w, part, r1, r2, (far, near, late) in (
            ("y", y, part_q, r1_q, r2_q, (PQ, IQ, LQ)),
            ("z", z, part_o, r1_o, r2_o, (PO, IO, LO)),
        ):
            up, down = on(axis, 1), on(axis, -1)
            flow(far, s, 1, (part(s, w + 2, 0), r1.at[s, 0], up))
            flow(far, s, -1, (part(s, w + 2, 1), r1.at[s, 1], down))
            flow(near, s, 1, (part(s, w + 1, 1), r2.at[s, 0, 1], up))
            flow(near, s, -1, (part(s, w - 1, 0), r2.at[s, 1, 0], down))
            flow(late, s, 1, (part(s, w + 1, 0), r2.at[s, 0, 0], up))
            flow(late, s, -1, (part(s, w - 1, 1), r2.at[s, 1, 1], down))
    home_q = out_q.at[features(z), :]
    home_o = out_o.at[:, lanes(y * 512, 512)]
    for s in range(3):
        flow(FQ, s, 0, (f_q.at[s], home_q, (row, x, order_q[s] * 4 + y)))
        flow(FO, s, 0, (f_o.at[s], home_o, (row, x, z * 4 + order_o[s])))

    def multiply_q(s):
        j = order_q[s]

        @pl.loop(0, 2)
        def _(n):
            right = vb_q[:, :, lanes(j * 512 + n * 256, 256)].reshape(2048, 256)
            total = jnp.dot(at_q[...], right, preferred_element_type=F32)
            for c in (0, 1):
                for h in (0, 1):
                    c_q[j, 2 * n + c, h] = total[h * 288:(h + 1) * 288, c * 128:(c + 1) * 128]

    def multiply_o(first):
        slots, k = (slice(0, 2), slice(0, 1024)) if first else (slice(2, 4), slice(1024, 2048))

        @pl.loop(0, 4)
        def _(w):
            for h in (0, 1):
                right = va_o[slots, :, :, h * 256:(h + 1) * 256].reshape(1024, 256)
                total = jnp.dot(bt_o[w, :, k], right, preferred_element_type=F32)
                for j in range(4):
                    part = total[j * 72:(j + 1) * 72]
                    c_o[w, j, h] = part if first else c_o[w, j, h] + part

    def join(s, w, part, r1):
        for ref, k in ((part(s, w + 1, 0), 0), (part(s, w - 1, 1), 1)):
            ref[...] = ref[...] + r1[s, k]

    def join_q(s):
        join(s, y, part_q, r1_q)

    def join_o(s):
        join(s, z, part_o, r1_o)

    def finish_q(s):
        for h in (0, 1):
            rows = slice(h * 288, (h + 1) * 288)
            total = part_q(s, y, h)[...] + r2_q[s, 0, h] + r2_q[s, 1, h]
            if s < 3:
                f_q[s, rows] = total
            else:
                out_q[pl.ds(pl.multiple_of(z * 576 + h * 288, 32), 288)] = total

    def finish_o(s):
        for h in (0, 1):
            total = part_o(s, z, h)[...] + r2_o[s, 0, h] + r2_o[s, 1, h]
            if s < 3:
                f_o[s, :, h * 256:(h + 1) * 256] = total
            else:
                out_o[:, lanes(y * 512 + h * 256, 256)] = total

    whole = {}
    for s in range(4):
        for p, i, l, r1, r2 in ((PQ, IQ, LQ, r1_q, r2_q), (PO, IO, LO, r1_o, r2_o)):
            far, rest = r1.at[s], r2.at[s]
            for step in (1, -1):
                whole[p, s, step] = far
                whole[i, s, step] = whole[l, s, step] = rest
    for p in (2, 3):
        whole[AQ, p, 0] = vb_q.at[1:4, mine, lanes(order_q[p] * 512, 512)]
    copies, arrivals, free = {}, {}, list(range(N_SEND))
    open_left, open_came = {}, {}

    def send(*names):
        for name in names:
            copies[name] = []
            for src, dst, device in flows[name]:
                group = id(whole[name]) if name in whole else (name, len(copies[name]))
                arrival = arrivals.setdefault(group, len(arrivals))
                k = free.pop(0)
                copy = pltpu.make_async_remote_copy(
                    src, dst, ssem.at[k], rsem.at[arrival], device_id=device, device_id_type=MESH
                )
                copy.start()
                copies[name].append((copy, k))
            open_left[name] = open_came[name] = True

    def left(*names):
        for name in names:
            del open_left[name]
            for copy, k in copies[name]:
                copy.wait_send()
                free.append(k)

    def came(*names):
        for name in names:
            if name not in open_came:
                continue
            if name in whole:
                both = whole[name]
                arrival = arrivals[id(both)]
                pltpu.make_async_remote_copy(
                    both, both, ssem.at[0], rsem.at[arrival], device_id=sibling, device_id_type=MESH
                ).wait_recv()
                for other in whole:
                    if whole[other] is both:
                        del open_came[other]
            else:
                del open_came[name]
                for copy, _ in copies[name]:
                    copy.wait_recv()

    send((EXQ, 1, 0), (EXQ, 2, 0))
    send((GQ, 0, 1), (GQ, 0, -1))
    send((EXO, 3, 0))
    left((EXQ, 1, 0), (EXQ, 2, 0))
    send((EXQ, 3, 0))
    came((EXQ, 2, 0))
    send((GQ, 2, 1), (GQ, 2, -1))
    left((EXO, 3, 0))
    send((DO, 0, 1), (DO, 0, -1))
    left((GQ, 0, 1), (GQ, 0, -1))
    left((EXQ, 3, 0))
    send((DQ, 0, 1), (DQ, 0, -1))
    send((EXO, 1, 0), (EXO, 2, 0))
    came((EXQ, 1, 0))
    send((GQ, 1, 1), (GQ, 1, -1))
    left((GQ, 2, 1))
    came((EXQ, 3, 0))
    send((GQ, 3, 1), (GQ, 3, -1))
    send((OWNQ, 0, 0), (OWNO, 0, 0))
    send((DQ, 1, 2))
    left((DQ, 0, -1))
    send((DQ, 1, -1))
    left((GQ, 2, -1))
    came((DQ, 0, -1))
    send((RQ, 1, 0))
    send((DQ, 1, 3))
    came((GQ, 2, 1), (GQ, 2, -1))
    send((HQ, 2, 1), (HQ, 2, -1))
    left((EXO, 1, 0), (EXO, 2, 0), (GQ, 1, 1), (GQ, 1, -1))
    came((GQ, 1, -1))
    send((HQ, 1, -1))
    came((EXO, 1, 0))
    send((GO, 1, 1), (GO, 1, -1))
    came((GQ, 0, 1))
    send((HQ, 0, 1))
    left((OWNO, 0, 0))
    left((DO, 0, 1), (DO, 0, -1))
    send((DO, 1, 1), (DO, 1, -1))
    came((DQ, 1, 2))
    send((RQ, 0, 0))
    came((DO, 0, 1), (DO, 0, -1))
    send((RO, 0, 1), (RO, 0, -1), (AO, 0, 0))
    left((DQ, 0, 1), (GQ, 3, -1), (OWNQ, 0, 0), (DQ, 1, 2))
    came((DQ, 1, 3))
    send((RQ, 0, 1), (AQ, 1, 1))
    send((GO, 0, 1), (GO, 0, -1))
    came((DQ, 0, 1))
    send((AQ, 0, 1), (AQ, 0, 2))
    came((GQ, 3, 1), (GQ, 3, -1))
    send((HQ, 3, 1), (HQ, 3, -1))
    left((DQ, 1, 3), (HQ, 2, 1), (HQ, 2, -1))
    came((DQ, 1, -1))
    send((AQ, 1, 2))
    came((RQ, 0, 0))
    send((AQ, 0, 4))
    left((RQ, 0, 1))
    send((RQ, 3, 1))
    left((RQ, 1, 0))
    send((RQ, 2, 0))
    left((GO, 1, -1), (AO, 0, 0), (AQ, 1, 1), (AQ, 0, 1), (AQ, 0, 2))
    came((RQ, 0, 1))
    send((AQ, 0, 5))
    left((RQ, 0, 0))
    send((DQ, 2, 1))
    left((GQ, 3, 1))
    came((EXO, 2, 0))
    send((GO, 2, 1), (GO, 2, -1))
    send((RQ, 3, 2))
    came((EXO, 3, 0))
    send((GO, 3, 1), (GO, 3, -1))
    left((DQ, 1, -1))
    send((DQ, 2, -1))
    left((HQ, 1, -1), (HQ, 0, 1), (DO, 1, 1), (DO, 1, -1), (RO, 0, 1), (RO, 0, -1))
    came((RQ, 1, 0))
    send((AQ, 1, 3))
    came((DO, 1, 1), (DO, 1, -1))
    send((RO, 1, 1), (RO, 1, -1), (AO, 1, 0))
    came((GQ, 0, -1), (HQ, 0, 1), (GQ, 1, 1), (HQ, 1, -1), (HQ, 2, 1), (HQ, 2, -1), (HQ, 3, 1), (HQ, 3, -1))
    came((AQ, 0, 1), (AQ, 0, 2), (AQ, 0, 4), (AQ, 0, 5), (OWNQ, 0, 0))
    multiply_q(0)
    send((PQ, 0, 1), (PQ, 0, -1))
    came((AQ, 1, 1), (AQ, 1, 2), (AQ, 1, 3))
    multiply_q(1)
    send((PQ, 1, 1), (PQ, 1, -1))
    came((GO, 1, -1))
    send((HO, 1, -1))
    left((GO, 0, 1), (GO, 0, -1), (HQ, 3, 1), (HQ, 3, -1), (AQ, 1, 2), (AQ, 0, 4))
    came((RO, 1, 1), (RO, 1, -1))
    send((AO, 3, 0))
    left((GO, 1, 1))
    came((GO, 0, 1))
    send((HO, 0, 1))
    left((AQ, 0, 5), (AQ, 1, 3), (RO, 1, 1), (RO, 1, -1), (AO, 1, 0))
    came((GO, 3, 1), (GO, 3, -1))
    send((HO, 3, 1), (HO, 3, -1))
    left((PQ, 0, 1))
    send((IQ, 0, 1), (IQ, 0, -1))
    came((RO, 0, 1), (RO, 0, -1))
    send((AO, 2, 0))
    left((RQ, 3, 1), (GO, 2, 1), (GO, 2, -1), (RQ, 3, 2), (GO, 3, 1), (GO, 3, -1), (AO, 3, 0))
    left((DQ, 2, -1))
    send((DQ, 3, -1))
    send((IQ, 1, 1), (IQ, 1, -1))
    left((DQ, 2, 1))
    send((DQ, 3, 1))
    came((GO, 2, 1), (GO, 2, -1))
    send((HO, 2, 1), (HO, 2, -1))
    left((RQ, 2, 0), (PQ, 0, -1))
    came((OWNO, 0, 0), (AO, 0, 0), (AO, 1, 0), (AO, 2, 0), (AO, 3, 0), (GO, 0, -1), (HO, 0, 1), (GO, 1, 1))
    came((HO, 1, -1))
    multiply_o(True)
    came((DQ, 2, 1), (DQ, 2, -1), (RQ, 2, 0))
    send((AQ, 2, 0))
    came((PQ, 0, 1), (PQ, 0, -1))
    join_q(0)
    send((LQ, 0, 1), (LQ, 0, -1))
    left((PQ, 1, 1), (PQ, 1, -1), (HO, 1, -1), (HO, 0, 1), (HO, 3, 1), (HO, 3, -1), (AO, 2, 0), (HO, 2, 1))
    left((HO, 2, -1))
    came((HO, 2, 1), (HO, 2, -1), (HO, 3, 1), (HO, 3, -1))
    multiply_o(False)
    send((PO, 2, 1), (PO, 2, -1))
    send((PO, 3, 1), (PO, 3, -1))
    send((IO, 3, 1), (IO, 3, -1))
    came((PQ, 1, 1), (PQ, 1, -1))
    join_q(1)
    send((LQ, 1, 1), (LQ, 1, -1))
    came((DQ, 3, 1), (DQ, 3, -1), (RQ, 3, 1), (RQ, 3, 2))
    send((AQ, 3, 0))
    came((AQ, 2, 0))
    multiply_q(2)
    send((PQ, 2, 1), (PQ, 2, -1))
    send((PO, 0, 1), (PO, 0, -1))
    left((IQ, 0, 1), (IQ, 0, -1), (DQ, 3, -1), (IQ, 1, 1), (IQ, 1, -1), (DQ, 3, 1), (AQ, 2, 0))
    left((PO, 2, 1))
    send((IO, 2, 1), (IO, 2, -1))
    came((PO, 3, 1), (PO, 3, -1))
    join_o(3)
    send((LO, 3, 1), (LO, 3, -1))
    came((AQ, 3, 0))
    multiply_q(3)
    send((PQ, 3, 1), (PQ, 3, -1))
    send((IQ, 2, 1), (IQ, 2, -1))
    left((PO, 0, 1))
    send((PO, 1, 1), (PO, 1, -1))
    left((LQ, 0, 1), (LQ, 0, -1), (PO, 2, -1), (PO, 3, 1), (PO, 3, -1), (IO, 3, 1), (IO, 3, -1), (AQ, 3, 0))
    left((PO, 0, -1))
    came((IQ, 1, 1), (IQ, 1, -1), (LQ, 1, 1), (LQ, 1, -1))
    finish_q(1)
    send((FQ, 1, 0))
    came((PO, 0, 1), (PO, 0, -1))
    join_o(0)
    send((LO, 0, 1), (LO, 0, -1))
    came((PO, 2, 1), (PO, 2, -1))
    join_o(2)
    send((LO, 2, 1), (LO, 2, -1))
    left((LQ, 1, 1), (LQ, 1, -1), (IO, 2, 1), (IO, 2, -1))
    came((IO, 3, 1), (IO, 3, -1), (LO, 3, 1), (LO, 3, -1))
    finish_o(3)
    left((PQ, 2, 1), (PQ, 2, -1), (LO, 3, 1), (LO, 3, -1))
    came((PQ, 2, 1), (PQ, 2, -1))
    join_q(2)
    send((LQ, 2, 1), (LQ, 2, -1))
    send((IO, 0, 1), (IO, 0, -1))
    send((IO, 1, 1), (IO, 1, -1))
    came((PO, 1, 1), (PO, 1, -1))
    join_o(1)
    send((LO, 1, 1), (LO, 1, -1))
    left((PO, 1, 1), (PO, 1, -1))
    left((PQ, 3, 1))
    send((IQ, 3, 1), (IQ, 3, -1))
    came((IQ, 0, 1), (IQ, 0, -1), (LQ, 0, 1), (LQ, 0, -1))
    finish_q(0)
    send((FQ, 0, 0))
    came((PQ, 3, 1), (PQ, 3, -1))
    join_q(3)
    send((LQ, 3, 1), (LQ, 3, -1))
    left((PQ, 3, -1), (IQ, 2, 1), (IQ, 2, -1), (LO, 0, 1), (LO, 0, -1), (LO, 2, 1), (LO, 2, -1))
    came((IQ, 2, 1), (IQ, 2, -1), (LQ, 2, 1), (LQ, 2, -1))
    finish_q(2)
    send((FQ, 2, 0))
    left((LQ, 2, 1), (LQ, 2, -1), (IO, 0, 1), (IO, 0, -1), (IO, 1, 1), (IO, 1, -1))
    came((IO, 1, 1), (IO, 1, -1), (LO, 1, 1), (LO, 1, -1))
    finish_o(1)
    send((FO, 1, 0))
    came((IO, 0, 1), (IO, 0, -1), (LO, 0, 1), (LO, 0, -1))
    finish_o(0)
    send((FO, 0, 0))
    came((IO, 2, 1), (IO, 2, -1), (LO, 2, 1), (LO, 2, -1))
    finish_o(2)
    send((FO, 2, 0))
    left((LO, 1, 1), (LO, 1, -1))
    came((IQ, 3, 1), (IQ, 3, -1), (LQ, 3, 1), (LQ, 3, -1))
    finish_q(3)

    came(*list(open_came))
    left(*list(open_left))
    assert len(arrivals) == N_COME and len(locals_) == 7, len(arrivals)


def per_device(normed, qkv_grad, attn_out, out_grad):
    flat = [v.reshape(v.shape[0] * v.shape[1], v.shape[2]) for v in (normed, qkv_grad, attn_out, out_grad)]
    hbm = pl.BlockSpec(memory_space=pltpu.HBM)
    vmem = pl.BlockSpec(memory_space=pltpu.VMEM)
    out_q, out_o = pl.pallas_call(
        kernel,
        out_shape=(
            jax.ShapeDtypeStruct((2304, 128), F32),
            jax.ShapeDtypeStruct((72, 2048), F32),
        ),
        in_specs=[hbm] * 4,
        out_specs=[vmem] * 2,
        scratch_shapes=[
            pltpu.VMEM((128, 2304), BF16),
            pltpu.VMEM((2304, 128), BF16),
            pltpu.VMEM((576, 2048), BF16),
            pltpu.VMEM((4, 512, 2048), BF16),
            pltpu.VMEM((4, 4, 2, 288, 128), F32),
            pltpu.VMEM((4, 2, 288, 128), F32),
            pltpu.VMEM((4, 2, 2, 288, 128), F32),
            pltpu.VMEM((3, 576, 128), F32),
            pltpu.VMEM((3, 128, 512), BF16),
            pltpu.VMEM((4, 4, 128, 512), BF16),
            pltpu.VMEM((256, 1152), BF16),
            pltpu.VMEM((4, 288, 2048), BF16),
            pltpu.VMEM((4, 4, 2, 72, 256), F32),
            pltpu.VMEM((4, 2, 72, 256), F32),
            pltpu.VMEM((4, 2, 2, 72, 256), F32),
            pltpu.VMEM((3, 72, 512), F32),
            pltpu.SemaphoreType.DMA((N_SEND,)),
            pltpu.SemaphoreType.DMA((N_COME,)),
            pltpu.SemaphoreType.DMA((7,)),
        ],
        compiler_params=pltpu.CompilerParams(
            collective_id=0, has_side_effects=True, vmem_limit_bytes=40 * 1024 * 1024
        ),
        name="weight_grads",
    )(*[pltpu.with_memory_space_constraint(v, pltpu.HBM) for v in flat])
    return out_q, out_o.T


def solution(mesh):
    in_specs = (
        P("col", "depth", "row"),
        P("row", "depth", "col"),
        P("col", "depth", "row"),
        P("row", "depth", "col"),
    )
    out_specs = (P("row", ("col", "depth")), P("row", ("col", "depth")))
    return jax.shard_map(
        per_device, mesh=mesh, in_specs=in_specs, out_specs=out_specs, check_vma=False
    )
```

```python
import jax
import jax.numpy as jnp
from jax import lax
from jax.experimental import pallas as pl
from jax.experimental.pallas import tpu as pltpu
from jax.sharding import PartitionSpec as P

MESH = pl.DeviceIdType.MESH
F32 = jnp.float32
BF16 = jnp.bfloat16

(EXQ, EXO, GQ, GO, HQ, HO, OWNQ, OWNO, DQ, DO, RQ, RO, AQ, AO, PQ, PO, IQ, IO, LQ, LO, FQ, FO) = range(22)
STEP = {1: 1, 2: -1, 3: 2}
N_SEND, N_COME = 26, 96


def kernel(
    a_q, b_q, a_o, b_o, out_q, out_o,
    la_q, ta_q, at_q, vb_q, c_q, r1_q, r2_q, f_q,
    sa_o, va_o, lb_o, bt_o, c_o, r1_o, r2_o, f_o,
    ssem, rsem, lsem,
):
    row, x, depth = lax.axis_index("row"), lax.axis_index("col"), lax.axis_index("depth")
    z, y = depth // 4, depth % 4

    def at(dx=0, dy=0, dz=0):
        return (row, (x + dx + 4) % 4, ((z + dz + 4) % 4) * 4 + (y + dy + 4) % 4)

    def on(axis, step):
        return at(**{"d" + axis: step})

    sibling = (1 - row, x, depth)

    barrier = pltpu.get_barrier_semaphore()
    peers = [sibling, at(dx=1), at(dx=-1)]
    for axis in "yz":
        peers += [on(axis, 1), on(axis, -1), on(axis, 2)]
    for peer in peers:
        pl.semaphore_signal(barrier, inc=1, device_id=peer, device_id_type=MESH)

    locals_ = []

    def local(src, dst):
        copy = pltpu.make_async_copy(src, dst, lsem.at[len(locals_)])
        copy.start()
        locals_.append(copy)
        return copy

    def lanes(start, size=128):
        return pl.ds(pl.multiple_of(start, 128), size)

    mine = lanes(row * 256, 256)
    load_la_q = local(a_q, la_q)
    load_lb_o = local(b_o, lb_o)
    loads = [local(b_q, vb_q.at[0, mine, :])]
    for d in (1, 2, 3):
        to = (y + STEP[d] + 4) % 4
        loads.append(local(a_o.at[:, lanes(to * 512, 512)], sa_o.at[d - 1]))
    loads.append(local(a_o.at[:, lanes(y * 512, 512)], va_o.at[0, x]))

    def features(u):
        return pl.ds(pl.multiple_of((u + 4) % 4 * 576, 64), 576)

    load_la_q.wait()
    ta_q[...] = la_q[...].T
    at_q[:, lanes(x * 128)] = ta_q[features(z), :]
    load_lb_o.wait()
    bt_o[:, :, lanes(row * 256, 256)] = lb_o[...].T.reshape(4, 288, 256)
    for copy in loads:
        copy.wait()
    pl.semaphore_wait(barrier, len(peers))

    flows = {}

    def flow(kind, number, which, *pieces):
        flows[kind, number, which] = pieces

    ahead, behind = (x + 1) % 4, (x + 3) % 4

    def piece_q(s, c):
        return at_q.at[:, lanes(s * 512 + c * 128)]

    for d in (1, 2, 3):
        flow(EXQ, d, 0, (ta_q.at[features(z + STEP[d]), :], piece_q(d, x), on("z", STEP[d])))
        flow(EXO, d, 0, (sa_o.at[d - 1], va_o.at[d, x], on("y", STEP[d])))
    for s in range(4):
        for step in (1, -1):
            src = ta_q.at[features(z), :] if s == 0 else piece_q(s, x)
            flow(GQ, s, step, (src, piece_q(s, x), at(dx=step)))
            flow(GO, s, step, (va_o.at[s, x], va_o.at[s, x], at(dx=step)))
            came_from = behind if step == 1 else ahead
            if s < 2:
                part_q, part_o = piece_q(s, came_from), va_o.at[s, came_from]
            else:
                half = slice(0, 288) if step == 1 else slice(288, 576)
                part_q = at_q.at[half, lanes(s * 512 + came_from * 128)]
                half = slice(0, 64) if step == 1 else slice(64, 128)
                part_o = va_o.at[s, came_from, half]
            flow(HQ, s, step, (part_q, part_q, at(dx=step)))
            flow(HO, s, step, (part_o, part_o, at(dx=step)))

    order_q = [(z + 1 + s) % 4 for s in range(4)]
    halves = [lanes(row * 256 + h * 128, 128) for h in (0, 1)]

    def strip(d, rows, j):
        return vb_q.at[d, rows, lanes((j + 4) % 4 * 512, 512)]

    def same(part, device):
        return (part, part, device)

    for p in range(4):
        flow(DQ, p, 1, (strip(0, mine, z + 2 + p), strip(1, mine, z + 2 + p), at(dz=1)))
        flow(DQ, p, -1, (strip(0, mine, z + p), strip(2, mine, z + p), at(dz=-1)))
        for d in (1, 2, 3):
            flow(AQ, p, d, same(strip(d, mine, order_q[p]), sibling))
        flow(AQ, p, 0, *[same(strip(d, mine, order_q[p]), sibling) for d in (1, 2, 3)])
    for h in (0, 1):
        flow(DQ, 1, h + 2, (strip(0, halves[h], z + 3), strip(1, halves[h], z + 3), at(dz=1)))
        flow(RQ, 0, h, (strip(1, halves[h], z + 2), strip(3, halves[h], z + 2), at(dz=1)))
        flow(AQ, 0, h + 4, same(strip(3, halves[h], order_q[0]), sibling))
    flow(RQ, 3, 1, (strip(1, halves[0], z + 1), strip(3, halves[0], z + 1), at(dz=1)))
    flow(RQ, 3, 2, (strip(1, halves[1], z + 1), strip(3, halves[1], z + 1), at(dz=1)))
    flow(RQ, 1, 0, (strip(2, mine, z + 1), strip(3, mine, z + 1), at(dz=-1)))
    flow(RQ, 2, 0, (strip(2, mine, z + 2), strip(3, mine, z + 2), at(dz=-1)))
    flow(OWNQ, 0, 0, same(vb_q.at[0, mine, :], sibling))

    def turned(d, p, first=0, size=256):
        return bt_o.at[2 * p:2 * p + 2, :, lanes(d * 512 + row * 256 + first, size)]

    for p in (0, 1):
        for d in (1, 2):
            flow(DO, p, STEP[d], (turned(0, p), turned(d, p), at(dy=STEP[d])))
            first = (d - 1) * 128
            flow(RO, p, STEP[d], (turned(d, p, first, 128), turned(3, p, first, 128), at(dy=STEP[d])))
        flow(AO, p, 0, same(turned(1, p), sibling), same(turned(2, p), sibling))
        flow(AO, p + 2, 0, same(turned(3, p), sibling))
    own = bt_o.at[:, :, lanes(row * 256, 256)]
    flow(OWNO, 0, 0, same(own, sibling))

    order_o = [(y + 1 + s) % 4 for s in range(4)]

    def part_q(s, w, h):
        return c_q.at[order_q[s], (w + 4) % 4, h]

    def part_o(s, w, h):
        return c_o.at[(w + 4) % 4, order_o[s], h]

    for s in range(4):
        for axis, w, part, r1, r2, (far, near, late) in (
            ("y", y, part_q, r1_q, r2_q, (PQ, IQ, LQ)),
            ("z", z, part_o, r1_o, r2_o, (PO, IO, LO)),
        ):
            up, down = on(axis, 1), on(axis, -1)
            flow(far, s, 1, (part(s, w + 2, 0), r1.at[s, 0], up))
            flow(far, s, -1, (part(s, w + 2, 1), r1.at[s, 1], down))
            flow(near, s, 1, (part(s, w + 1, 1), r2.at[s, 0, 1], up))
            flow(near, s, -1, (part(s, w - 1, 0), r2.at[s, 1, 0], down))
            flow(late, s, 1, (part(s, w + 1, 0), r2.at[s, 0, 0], up))
            flow(late, s, -1, (part(s, w - 1, 1), r2.at[s, 1, 1], down))
    home_q = out_q.at[features(z), :]
    home_o = out_o.at[:, lanes(y * 512, 512)]
    for s in range(3):
        flow(FQ, s, 0, (f_q.at[s], home_q, (row, x, order_q[s] * 4 + y)))
        flow(FO, s, 0, (f_o.at[s], home_o, (row, x, z * 4 + order_o[s])))

    def multiply_q(s):
        j = order_q[s]

        @pl.loop(0, 2)
        def _(n):
            right = vb_q[:, :, lanes(j * 512 + n * 256, 256)].reshape(2048, 256)
            total = jnp.dot(at_q[...], right, preferred_element_type=F32)
            for c in (0, 1):
                for h in (0, 1):
                    c_q[j, 2 * n + c, h] = total[h * 288:(h + 1) * 288, c * 128:(c + 1) * 128]

    def multiply_o(first):
        slots, k = (slice(0, 2), slice(0, 1024)) if first else (slice(2, 4), slice(1024, 2048))

        @pl.loop(0, 4)
        def _(w):
            for h in (0, 1):
                right = va_o[slots, :, :, h * 256:(h + 1) * 256].reshape(1024, 256)
                total = jnp.dot(bt_o[w, :, k], right, preferred_element_type=F32)
                for j in range(4):
                    part = total[j * 72:(j + 1) * 72]
                    c_o[w, j, h] = part if first else c_o[w, j, h] + part

    def join(s, w, part, r1):
        for ref, k in ((part(s, w + 1, 0), 0), (part(s, w - 1, 1), 1)):
            ref[...] = ref[...] + r1[s, k]

    def join_q(s):
        join(s, y, part_q, r1_q)

    def join_o(s):
        join(s, z, part_o, r1_o)

    def finish_q(s):
        for h in (0, 1):
            rows = slice(h * 288, (h + 1) * 288)
            total = part_q(s, y, h)[...] + r2_q[s, 0, h] + r2_q[s, 1, h]
            if s < 3:
                f_q[s, rows] = total
            else:
                out_q[pl.ds(pl.multiple_of(z * 576 + h * 288, 32), 288)] = total

    def finish_o(s):
        for h in (0, 1):
            total = part_o(s, z, h)[...] + r2_o[s, 0, h] + r2_o[s, 1, h]
            if s < 3:
                f_o[s, :, h * 256:(h + 1) * 256] = total
            else:
                out_o[:, lanes(y * 512 + h * 256, 256)] = total

    whole = {}
    for s in range(4):
        for p, i, l, r1, r2 in ((PQ, IQ, LQ, r1_q, r2_q), (PO, IO, LO, r1_o, r2_o)):
            far, rest = r1.at[s], r2.at[s]
            for step in (1, -1):
                whole[p, s, step] = far
                whole[i, s, step] = whole[l, s, step] = rest
    for p in (2, 3):
        whole[AQ, p, 0] = vb_q.at[1:4, mine, lanes(order_q[p] * 512, 512)]
    copies, arrivals, free = {}, {}, list(range(N_SEND))
    open_left, open_came = {}, {}

    def send(*names):
        for name in names:
            copies[name] = []
            for src, dst, device in flows[name]:
                group = id(whole[name]) if name in whole else (name, len(copies[name]))
                arrival = arrivals.setdefault(group, len(arrivals))
                k = free.pop(0)
                copy = pltpu.make_async_remote_copy(
                    src, dst, ssem.at[k], rsem.at[arrival], device_id=device, device_id_type=MESH
                )
                copy.start()
                copies[name].append((copy, k))
            open_left[name] = open_came[name] = True

    def left(*names):
        for name in names:
            del open_left[name]
            for copy, k in copies[name]:
                copy.wait_send()
                free.append(k)

    def came(*names):
        for name in names:
            if name not in open_came:
                continue
            if name in whole:
                both = whole[name]
                arrival = arrivals[id(both)]
                pltpu.make_async_remote_copy(
                    both, both, ssem.at[0], rsem.at[arrival], device_id=sibling, device_id_type=MESH
                ).wait_recv()
                for other in whole:
                    if whole[other] is both:
                        del open_came[other]
            else:
                del open_came[name]
                for copy, _ in copies[name]:
                    copy.wait_recv()

    send((OWNQ, 0, 0), (OWNO, 0, 0))
    send((EXO, 1, 0), (EXO, 2, 0))
    send((EXQ, 1, 0), (EXQ, 2, 0))
    send((GQ, 0, 1), (GQ, 0, -1))
    left((EXO, 1, 0), (EXO, 2, 0))
    send((EXO, 3, 0))
    left((EXQ, 1, 0), (EXQ, 2, 0))
    send((EXQ, 3, 0))
    left((GQ, 0, 1))
    came((EXQ, 1, 0))
    send((GQ, 1, 1), (GQ, 1, -1))
    send((DQ, 0, 1), (DQ, 0, -1))
    left((OWNO, 0, 0), (GQ, 0, -1))
    left((EXO, 3, 0))
    send((DO, 0, 1), (DO, 0, -1))
    came((EXQ, 2, 0))
    send((GQ, 2, 1), (GQ, 2, -1))
    left((OWNQ, 0, 0))
    left((GQ, 1, 1))
    came((EXQ, 3, 0))
    send((GQ, 3, 1), (GQ, 3, -1))
    send((DQ, 1, 2))
    left((EXQ, 3, 0))
    left((DQ, 0, -1))
    send((DQ, 1, -1))
    came((GQ, 0, 1))
    send((HQ, 0, 1))
    left((GQ, 1, -1))
    came((GQ, 2, 1), (GQ, 2, -1))
    send((HQ, 2, 1), (HQ, 2, -1))
    send((DQ, 1, 3))
    send((GO, 0, 1), (GO, 0, -1))
    left((DO, 0, 1), (DO, 0, -1))
    send((DO, 1, 1), (DO, 1, -1))
    left((GQ, 2, 1))
    came((GQ, 1, -1))
    send((HQ, 1, -1))
    left((GQ, 2, -1))
    came((DQ, 1, 2))
    send((RQ, 0, 0))
    came((DQ, 0, -1))
    send((RQ, 1, 0))
    came((DQ, 0, 1))
    send((AQ, 0, 1), (AQ, 0, 2))
    left((DQ, 0, 1), (GQ, 3, -1), (DQ, 1, 2))
    came((DQ, 1, 3))
    send((RQ, 0, 1), (AQ, 1, 1))
    came((DO, 0, 1), (DO, 0, -1))
    send((RO, 0, 1), (RO, 0, -1), (AO, 0, 0))
    came((EXO, 1, 0))
    send((GO, 1, 1), (GO, 1, -1))
    left((DQ, 1, 3))
    came((GQ, 3, 1), (GQ, 3, -1))
    send((HQ, 3, 1), (HQ, 3, -1))
    left((GQ, 3, 1), (HQ, 2, -1), (DO, 1, 1), (DO, 1, -1), (AQ, 0, 1), (AQ, 0, 2))
    came((RQ, 0, 0))
    send((AQ, 0, 4))
    came((DO, 1, 1), (DO, 1, -1))
    send((RO, 1, 1), (RO, 1, -1), (AO, 1, 0))
    left((HQ, 2, 1), (RQ, 0, 0), (AQ, 1, 1))
    left((DQ, 1, -1), (RQ, 1, 0))
    send((DQ, 2, -1))
    left((RQ, 0, 1))
    send((RQ, 3, 1))
    left((AO, 0, 0))
    came((RQ, 0, 1))
    send((AQ, 0, 5))
    came((EXO, 2, 0))
    send((GO, 2, 1), (GO, 2, -1))
    came((DQ, 1, -1))
    send((RQ, 2, 0))
    left((HQ, 0, 1), (GO, 0, 1), (GO, 0, -1), (HQ, 1, -1), (RO, 0, 1), (RO, 0, -1))
    left((RQ, 3, 1))
    send((DQ, 2, 1))
    send((AQ, 1, 2))
    send((RQ, 3, 2))
    came((RQ, 1, 0))
    send((AQ, 1, 3))
    came((EXO, 3, 0))
    send((GO, 3, 1), (GO, 3, -1))
    came((GQ, 0, -1), (HQ, 0, 1), (GQ, 1, 1), (HQ, 1, -1), (HQ, 2, 1), (HQ, 2, -1), (HQ, 3, 1), (HQ, 3, -1))
    came((AQ, 0, 1), (AQ, 0, 2), (AQ, 0, 4), (AQ, 0, 5), (OWNQ, 0, 0))
    multiply_q(0)
    send((PQ, 0, 1), (PQ, 0, -1))
    left((GO, 1, -1), (HQ, 3, 1), (HQ, 3, -1), (AQ, 0, 4), (RO, 1, 1), (RO, 1, -1), (AO, 1, 0), (AQ, 0, 5))
    came((AQ, 1, 1), (AQ, 1, 2), (AQ, 1, 3))
    multiply_q(1)
    send((PQ, 1, 1), (PQ, 1, -1))
    left((GO, 1, 1))
    came((GO, 0, 1))
    send((HO, 0, 1))
    left((GO, 2, 1))
    came((GO, 1, -1))
    send((HO, 1, -1))
    came((RO, 0, 1), (RO, 0, -1))
    send((AO, 2, 0))
    came((RO, 1, 1), (RO, 1, -1))
    send((AO, 3, 0))
    left((AQ, 1, 2), (AQ, 1, 3))
    left((DQ, 2, -1))
    send((DQ, 3, -1))
    left((PQ, 0, 1))
    send((IQ, 0, 1), (IQ, 0, -1))
    send((IQ, 1, 1), (IQ, 1, -1))
    came((GO, 3, 1), (GO, 3, -1))
    send((HO, 3, 1), (HO, 3, -1))
    left((GO, 2, -1), (GO, 3, -1))
    left((DQ, 2, 1))
    send((DQ, 3, 1))
    left((GO, 3, 1))
    came((GO, 2, 1), (GO, 2, -1))
    send((HO, 2, 1), (HO, 2, -1))
    left((RQ, 3, 2), (PQ, 0, -1), (AO, 2, 0), (AO, 3, 0))
    came((OWNO, 0, 0), (AO, 0, 0), (AO, 1, 0), (AO, 2, 0), (AO, 3, 0), (GO, 0, -1), (HO, 0, 1), (GO, 1, 1))
    came((HO, 1, -1))
    multiply_o(True)
    came((DQ, 2, 1), (DQ, 2, -1), (RQ, 2, 0))
    send((AQ, 2, 0))
    left((RQ, 2, 0), (HO, 0, 1), (HO, 1, -1), (HO, 3, 1), (HO, 3, -1), (HO, 2, 1), (HO, 2, -1))
    came((HO, 2, 1), (HO, 2, -1), (HO, 3, 1), (HO, 3, -1))
    multiply_o(False)
    came((PQ, 1, 1), (PQ, 1, -1))
    join_q(1)
    send((LQ, 1, 1), (LQ, 1, -1))
    send((PO, 3, 1), (PO, 3, -1))
    send((IO, 3, 1), (IO, 3, -1))
    left((PQ, 1, 1), (PQ, 1, -1))
    came((AQ, 2, 0))
    multiply_q(2)
    send((PQ, 2, 1), (PQ, 2, -1))
    send((PO, 0, 1), (PO, 0, -1))
    came((DQ, 3, 1), (DQ, 3, -1), (RQ, 3, 1), (RQ, 3, 2))
    send((AQ, 3, 0))
    came((PQ, 0, 1), (PQ, 0, -1))
    join_q(0)
    send((LQ, 0, 1), (LQ, 0, -1))
    send((PO, 2, 1), (PO, 2, -1))
    left((DQ, 3, -1), (IQ, 0, 1), (IQ, 0, -1), (IQ, 1, 1), (IQ, 1, -1), (DQ, 3, 1), (AQ, 2, 0))
    came((PO, 3, 1), (PO, 3, -1))
    join_o(3)
    send((LO, 3, 1), (LO, 3, -1))
    left((LQ, 1, 1), (LQ, 1, -1), (PO, 3, 1), (PO, 3, -1), (IO, 3, 1), (IO, 3, -1))
    left((PO, 0, 1))
    send((PO, 1, 1), (PO, 1, -1))
    came((AQ, 3, 0))
    multiply_q(3)
    send((PQ, 3, 1), (PQ, 3, -1))
    came((IQ, 1, 1), (IQ, 1, -1), (LQ, 1, 1), (LQ, 1, -1))
    finish_q(1)
    send((FQ, 1, 0))
    send((IQ, 2, 1), (IQ, 2, -1))
    send((IO, 2, 1), (IO, 2, -1))
    left((PO, 0, -1), (AQ, 3, 0), (PO, 2, 1), (PO, 2, -1))
    came((IO, 3, 1), (IO, 3, -1), (LO, 3, 1), (LO, 3, -1))
    finish_o(3)
    came((PO, 0, 1), (PO, 0, -1))
    join_o(0)
    send((LO, 0, 1), (LO, 0, -1))
    left((LO, 3, 1), (LO, 3, -1))
    came((PQ, 2, 1), (PQ, 2, -1))
    join_q(2)
    send((LQ, 2, 1), (LQ, 2, -1))
    send((IO, 0, 1), (IO, 0, -1))
    send((IQ, 3, 1), (IQ, 3, -1))
    left((PO, 1, 1))
    send((IO, 1, 1), (IO, 1, -1))
    came((PO, 1, 1), (PO, 1, -1))
    join_o(1)
    send((LO, 1, 1), (LO, 1, -1))
    left((PQ, 2, 1), (PQ, 2, -1), (LQ, 0, 1), (LQ, 0, -1), (PO, 1, -1))
    came((PQ, 3, 1), (PQ, 3, -1))
    join_q(3)
    send((LQ, 3, 1), (LQ, 3, -1))
    came((PO, 2, 1), (PO, 2, -1))
    join_o(2)
    send((LO, 2, 1), (LO, 2, -1))
    left((PQ, 3, 1), (PQ, 3, -1), (IQ, 2, 1), (IQ, 2, -1), (IO, 2, 1), (IO, 2, -1), (LO, 0, 1), (LO, 0, -1))
    left((IO, 0, 1), (IO, 0, -1), (IO, 1, -1))
    came((IQ, 2, 1), (IQ, 2, -1), (LQ, 2, 1), (LQ, 2, -1))
    finish_q(2)
    send((FQ, 2, 0))
    came((IQ, 0, 1), (IQ, 0, -1), (LQ, 0, 1), (LQ, 0, -1))
    finish_q(0)
    send((FQ, 0, 0))
    came((IO, 0, 1), (IO, 0, -1), (LO, 0, 1), (LO, 0, -1))
    finish_o(0)
    send((FO, 0, 0))
    left((LQ, 2, 1), (LQ, 2, -1), (IQ, 3, 1), (IQ, 3, -1), (IO, 1, 1), (LO, 1, 1), (LO, 1, -1))
    came((IO, 2, 1), (IO, 2, -1), (LO, 2, 1), (LO, 2, -1))
    finish_o(2)
    send((FO, 2, 0))
    left((LQ, 3, -1), (LO, 2, 1), (LO, 2, -1))
    came((IQ, 3, 1), (IQ, 3, -1), (LQ, 3, 1), (LQ, 3, -1))
    finish_q(3)
    came((IO, 1, 1), (IO, 1, -1), (LO, 1, 1), (LO, 1, -1))
    finish_o(1)
    send((FO, 1, 0))

    came(*list(open_came))
    left(*list(open_left))
    assert len(arrivals) == N_COME and len(locals_) == 7, len(arrivals)


def store(q_ref, o_ref, out_q, out_o, sem):
    copies = [pltpu.make_async_copy(q_ref, out_q, sem.at[0]), pltpu.make_async_copy(o_ref, out_o, sem.at[1])]
    for copy in copies:
        copy.start()
    for copy in copies:
        copy.wait()


def per_device(normed, qkv_grad, attn_out, out_grad):
    flat = [v.reshape(v.shape[0] * v.shape[1], v.shape[2]) for v in (normed, qkv_grad, attn_out, out_grad)]
    hbm = pl.BlockSpec(memory_space=pltpu.HBM)
    vmem = pl.BlockSpec(memory_space=pltpu.VMEM)
    out_q, out_o = pl.pallas_call(
        kernel,
        out_shape=(
            jax.ShapeDtypeStruct((2304, 128), F32),
            jax.ShapeDtypeStruct((72, 2048), F32),
        ),
        in_specs=[hbm] * 4,
        out_specs=[vmem] * 2,
        scratch_shapes=[
            pltpu.VMEM((128, 2304), BF16),
            pltpu.VMEM((2304, 128), BF16),
            pltpu.VMEM((576, 2048), BF16),
            pltpu.VMEM((4, 512, 2048), BF16),
            pltpu.VMEM((4, 4, 2, 288, 128), F32),
            pltpu.VMEM((4, 2, 288, 128), F32),
            pltpu.VMEM((4, 2, 2, 288, 128), F32),
            pltpu.VMEM((3, 576, 128), F32),
            pltpu.VMEM((3, 128, 512), BF16),
            pltpu.VMEM((4, 4, 128, 512), BF16),
            pltpu.VMEM((256, 1152), BF16),
            pltpu.VMEM((4, 288, 2048), BF16),
            pltpu.VMEM((4, 4, 2, 72, 256), F32),
            pltpu.VMEM((4, 2, 72, 256), F32),
            pltpu.VMEM((4, 2, 2, 72, 256), F32),
            pltpu.VMEM((3, 72, 512), F32),
            pltpu.SemaphoreType.DMA((N_SEND,)),
            pltpu.SemaphoreType.DMA((N_COME,)),
            pltpu.SemaphoreType.DMA((7,)),
        ],
        compiler_params=pltpu.CompilerParams(
            collective_id=0, has_side_effects=True, vmem_limit_bytes=40 * 1024 * 1024
        ),
        name="weight_grads",
    )(*[pltpu.with_memory_space_constraint(v, pltpu.HBM) for v in flat])
    out_q, out_o = pl.pallas_call(
        store,
        out_shape=(
            jax.ShapeDtypeStruct((2304, 128), F32),
            jax.ShapeDtypeStruct((72, 2048), F32),
        ),
        in_specs=[vmem] * 2,
        out_specs=[hbm] * 2,
        scratch_shapes=[pltpu.SemaphoreType.DMA((2,))],
        compiler_params=pltpu.CompilerParams(vmem_limit_bytes=1024 * 1024),
        name="store",
    )(out_q, out_o)
    return out_q, out_o.T


def solution(mesh):
    in_specs = (
        P("col", "depth", "row"),
        P("row", "depth", "col"),
        P("col", "depth", "row"),
        P("row", "depth", "col"),
    )
    out_specs = (P("row", ("col", "depth")), P("row", ("col", "depth")))
    return jax.shard_map(
        per_device, mesh=mesh, in_specs=in_specs, out_specs=out_specs, check_vma=False
    )
```

```python
import jax
import jax.numpy as jnp
from jax import lax
from jax.experimental import pallas as pl
from jax.experimental.pallas import tpu as pltpu
from jax.sharding import PartitionSpec as P

MESH = pl.DeviceIdType.MESH
F32 = jnp.float32
BF16 = jnp.bfloat16

(EXQ, EXO, GQ, GO, HQ, HO, OWNQ, OWNO, DQ, DO, RQ, RO, AQ, AO, PQ, PO, IQ, IO, LQ, LO, FQ, FO) = range(22)
STEP = {1: 1, 2: -1, 3: 2}
N_SEND, N_COME = 24, 69


def kernel(
    a_q, b_q, a_o, b_o, out_q, out_o,
    la_q, ta_q, at_q, vb_q, c_q, r1_q, r2_q, f_q,
    sa_o, va_o, lb_o, bt_o, c_o, r1_o, r2_o, f_o,
    ssem, rsem, lsem,
):
    row, x, depth = lax.axis_index("row"), lax.axis_index("col"), lax.axis_index("depth")
    z, y = depth // 4, depth % 4

    def at(dx=0, dy=0, dz=0):
        return (row, (x + dx + 4) % 4, ((z + dz + 4) % 4) * 4 + (y + dy + 4) % 4)

    def on(axis, step):
        return at(**{"d" + axis: step})

    sibling = (1 - row, x, depth)

    barrier = pltpu.get_barrier_semaphore()
    peers = [sibling, at(dx=1), at(dx=-1)]
    for axis in "yz":
        peers += [on(axis, 1), on(axis, -1), on(axis, 2)]
    for peer in peers:
        pl.semaphore_signal(barrier, inc=1, device_id=peer, device_id_type=MESH)

    locals_ = []

    def local(src, dst):
        copy = pltpu.make_async_copy(src, dst, lsem.at[len(locals_)])
        copy.start()
        locals_.append(copy)
        return copy

    def lanes(start, size=128):
        return pl.ds(pl.multiple_of(start, 128), size)

    mine = lanes(row * 256, 256)
    load_la_q = local(a_q, la_q)
    load_lb_o = local(b_o, lb_o)
    loads = [local(b_q, vb_q.at[0, mine, :])]
    for d in (1, 2, 3):
        to = (y + STEP[d] + 4) % 4
        loads.append(local(a_o.at[:, lanes(to * 512, 512)], sa_o.at[d - 1]))
    loads.append(local(a_o.at[:, lanes(y * 512, 512)], va_o.at[0, x]))

    def features(u):
        return pl.ds(pl.multiple_of((u + 4) % 4 * 576, 64), 576)

    load_la_q.wait()
    ta_q[...] = la_q[...].T
    at_q[:, lanes(x * 128)] = ta_q[features(z), :]
    load_lb_o.wait()
    bt_o[:, :, lanes(row * 256, 256)] = lb_o[...].T.reshape(4, 288, 256)
    for copy in loads:
        copy.wait()
    pl.semaphore_wait(barrier, len(peers))

    flows = {}

    def flow(kind, number, which, *pieces):
        flows[kind, number, which] = pieces

    ahead, behind = (x + 1) % 4, (x + 3) % 4

    def piece_q(s, c):
        return at_q.at[:, lanes(s * 512 + c * 128)]

    for d in (1, 2, 3):
        flow(EXQ, d, 0, (ta_q.at[features(z + STEP[d]), :], piece_q(d, x), on("z", STEP[d])))
        flow(EXO, d, 0, (sa_o.at[d - 1], va_o.at[d, x], on("y", STEP[d])))
    for s in range(4):
        for step in (1, -1):
            src = ta_q.at[features(z), :] if s == 0 else piece_q(s, x)
            flow(GQ, s, step, (src, piece_q(s, x), at(dx=step)))
            flow(GO, s, step, (va_o.at[s, x], va_o.at[s, x], at(dx=step)))
            came_from = behind if step == 1 else ahead
            if s < 2:
                part_q, part_o = piece_q(s, came_from), va_o.at[s, came_from]
            else:
                half = slice(0, 288) if step == 1 else slice(288, 576)
                part_q = at_q.at[half, lanes(s * 512 + came_from * 128)]
                half = slice(0, 64) if step == 1 else slice(64, 128)
                part_o = va_o.at[s, came_from, half]
            flow(HQ, s, step, (part_q, part_q, at(dx=step)))
            flow(HO, s, step, (part_o, part_o, at(dx=step)))

    order_q = [(z + 1 + s) % 4 for s in range(4)]
    halves = [lanes(row * 256 + h * 128, 128) for h in (0, 1)]

    def strip(d, rows, j):
        return vb_q.at[d, rows, lanes((j + 4) % 4 * 512, 512)]

    def same(part, device):
        return (part, part, device)

    for p in range(4):
        flow(DQ, p, 1, (strip(0, mine, z + 2 + p), strip(1, mine, z + 2 + p), at(dz=1)))
        flow(DQ, p, -1, (strip(0, mine, z + p), strip(2, mine, z + p), at(dz=-1)))
        for d in (1, 2, 3):
            flow(AQ, p, d, same(strip(d, mine, order_q[p]), sibling))
        flow(AQ, p, 0, *[same(strip(d, mine, order_q[p]), sibling) for d in (1, 2, 3)])
    for h in (0, 1):
        flow(DQ, 1, h + 2, (strip(0, halves[h], z + 3), strip(1, halves[h], z + 3), at(dz=1)))
        flow(RQ, 0, h, (strip(1, halves[h], z + 2), strip(3, halves[h], z + 2), at(dz=1)))
        flow(AQ, 0, h + 4, same(strip(3, halves[h], order_q[0]), sibling))
    flow(RQ, 3, 1, (strip(1, halves[0], z + 1), strip(3, halves[0], z + 1), at(dz=1)))
    flow(RQ, 3, 2, (strip(1, halves[1], z + 1), strip(3, halves[1], z + 1), at(dz=1)))
    flow(RQ, 1, 0, (strip(2, mine, z + 1), strip(3, mine, z + 1), at(dz=-1)))
    flow(RQ, 2, 0, (strip(2, mine, z + 2), strip(3, mine, z + 2), at(dz=-1)))
    flow(OWNQ, 0, 0, same(vb_q.at[0, mine, :], sibling))

    def turned(d, p, first=0, size=256):
        return bt_o.at[2 * p:2 * p + 2, :, lanes(d * 512 + row * 256 + first, size)]

    for p in (0, 1):
        for d in (1, 2):
            flow(DO, p, STEP[d], (turned(0, p), turned(d, p), at(dy=STEP[d])))
            first = (d - 1) * 128
            flow(RO, p, STEP[d], (turned(d, p, first, 128), turned(3, p, first, 128), at(dy=STEP[d])))
        flow(AO, p, 0, same(turned(1, p), sibling), same(turned(2, p), sibling))
        flow(AO, p + 2, 0, same(turned(3, p), sibling))
    own = bt_o.at[:, :, lanes(row * 256, 256)]
    flow(OWNO, 0, 0, same(own, sibling))

    order_o = [(y + 1 + s) % 4 for s in range(4)]

    def part_q(s, w, h):
        return c_q.at[order_q[s], (w + 4) % 4, h]

    def part_o(s, w, h):
        return c_o.at[(w + 4) % 4, order_o[s], h]

    for s in range(4):
        for axis, w, part, r1, r2, (far, near, late) in (
            ("y", y, part_q, r1_q, r2_q, (PQ, IQ, LQ)),
            ("z", z, part_o, r1_o, r2_o, (PO, IO, LO)),
        ):
            up, down = on(axis, 1), on(axis, -1)
            flow(far, s, 1, (part(s, w + 2, 0), r1.at[s, 0], up))
            flow(far, s, -1, (part(s, w + 2, 1), r1.at[s, 1], down))
            flow(near, s, 1, (part(s, w + 1, 1), r2.at[s, 0, 1], up))
            flow(near, s, -1, (part(s, w - 1, 0), r2.at[s, 1, 0], down))
            flow(late, s, 1, (part(s, w + 1, 0), r2.at[s, 0, 0], up))
            flow(late, s, -1, (part(s, w - 1, 1), r2.at[s, 1, 1], down))
    home_q = out_q.at[features(z), :]
    home_o = out_o.at[:, lanes(y * 512, 512)]
    for s in range(3):
        flow(FQ, s, 0, (f_q.at[s], home_q, (row, x, order_q[s] * 4 + y)))
        flow(FO, s, 0, (f_o.at[s], home_o, (row, x, z * 4 + order_o[s])))

    def multiply_q(s):
        j = order_q[s]

        @pl.loop(0, 2)
        def _(n):
            right = vb_q[:, :, lanes(j * 512 + n * 256, 256)].reshape(2048, 256)
            total = jnp.dot(at_q[...], right, preferred_element_type=F32)
            for c in (0, 1):
                for h in (0, 1):
                    c_q[j, 2 * n + c, h] = total[h * 288:(h + 1) * 288, c * 128:(c + 1) * 128]

    def multiply_o(first):
        slots, k = (slice(0, 2), slice(0, 1024)) if first else (slice(2, 4), slice(1024, 2048))

        @pl.loop(0, 4)
        def _(w):
            for h in (0, 1):
                right = va_o[slots, :, :, h * 256:(h + 1) * 256].reshape(1024, 256)
                total = jnp.dot(bt_o[w, :, k], right, preferred_element_type=F32)
                for j in range(4):
                    part = total[j * 72:(j + 1) * 72]
                    c_o[w, j, h] = part if first else c_o[w, j, h] + part

    def join(s, w, part, r1):
        for ref, k in ((part(s, w + 1, 0), 0), (part(s, w - 1, 1), 1)):
            ref[...] = ref[...] + r1[s, k]

    def join_q(s):
        join(s, y, part_q, r1_q)

    def join_o(s):
        join(s, z, part_o, r1_o)

    def finish_q(s):
        for h in (0, 1):
            rows = slice(h * 288, (h + 1) * 288)
            total = part_q(s, y, h)[...] + r2_q[s, 0, h] + r2_q[s, 1, h]
            if s < 3:
                f_q[s, rows] = total
            else:
                out_q[pl.ds(pl.multiple_of(z * 576 + h * 288, 32), 288)] = total

    def finish_o(s):
        for h in (0, 1):
            total = part_o(s, z, h)[...] + r2_o[s, 0, h] + r2_o[s, 1, h]
            if s < 3:
                f_o[s, :, h * 256:(h + 1) * 256] = total
            else:
                out_o[:, lanes(y * 512 + h * 256, 256)] = total

    whole = {}
    for s in range(4):
        for p, i, l, r1, r2 in ((PQ, IQ, LQ, r1_q, r2_q), (PO, IO, LO, r1_o, r2_o)):
            far, rest = r1.at[s], r2.at[s]
            for step in (1, -1):
                whole[p, s, step] = far
                whole[i, s, step] = whole[l, s, step] = rest
    for p in (2, 3):
        whole[AQ, p, 0] = vb_q.at[1:4, mine, lanes(order_q[p] * 512, 512)]
    together = at_q.at[:, 0:768]
    for name in ((GQ, 0, -1), (HQ, 0, 1), (GQ, 1, 1), (HQ, 1, -1), (HQ, 2, 1), (HQ, 2, -1), (HQ, 3, 1), (HQ, 3, -1)):
        whole[name] = together
    together = va_o.at[0]
    for name in ((GO, 0, -1), (HO, 0, 1), (GO, 1, 1), (HO, 1, -1)):
        whole[name] = together
    together = va_o.at[2, 0:2]
    for name in ((HO, 2, 1), (HO, 2, -1), (HO, 3, 1), (HO, 3, -1)):
        whole[name] = together
    together = bt_o.at[:, :, 0:1024]
    for name in ((OWNO, 0, 0), (AO, 0, 0), (AO, 1, 0), (AO, 2, 0), (AO, 3, 0)):
        whole[name] = together
    for p in (0, 1):
        two = bt_o.at[2 * p:2 * p + 2, :, 0:512]
        one = bt_o.at[2 * p:2 * p + 2, :, 0:256]
        for step in (1, -1):
            whole[DO, p, step], whole[RO, p, step] = two, one
    three_q, three_o = out_q.at[0:1728], out_o.at[:, 0:1536]
    for s in range(3):
        whole[FQ, s, 0], whole[FO, s, 0] = three_q, three_o
    copies, arrivals, free = {}, {}, list(range(N_SEND))
    open_left, open_came = {}, {}

    def send(*names):
        for name in names:
            copies[name] = []
            for src, dst, device in flows[name]:
                group = id(whole[name]) if name in whole else (name, len(copies[name]))
                arrival = arrivals.setdefault(group, len(arrivals))
                k = free.pop(0)
                copy = pltpu.make_async_remote_copy(
                    src, dst, ssem.at[k], rsem.at[arrival], device_id=device, device_id_type=MESH
                )
                copy.start()
                copies[name].append((copy, k))
            open_left[name] = open_came[name] = True

    def left(*names):
        for name in names:
            del open_left[name]
            for copy, k in copies[name]:
                copy.wait_send()
                free.append(k)

    def came(*names):
        for name in names:
            if name not in open_came:
                continue
            if name in whole:
                both = whole[name]
                arrival = arrivals[id(both)]
                pltpu.make_async_remote_copy(
                    both, both, ssem.at[0], rsem.at[arrival], device_id=sibling, device_id_type=MESH
                ).wait_recv()
                for other in whole:
                    if whole[other] is both:
                        open_came.pop(other, None)
            else:
                del open_came[name]
                for copy, _ in copies[name]:
                    copy.wait_recv()

    send((OWNQ, 0, 0), (OWNO, 0, 0))
    send((EXO, 1, 0), (EXO, 2, 0))
    send((EXQ, 1, 0), (EXQ, 2, 0))
    send((GQ, 0, 1), (GQ, 0, -1))
    left((EXO, 1, 0), (EXO, 2, 0))
    send((EXO, 3, 0))
    left((EXQ, 1, 0), (EXQ, 2, 0))
    send((EXQ, 3, 0))
    left((GQ, 0, 1))
    came((EXQ, 1, 0))
    send((GQ, 1, 1), (GQ, 1, -1))
    send((DQ, 0, 1), (DQ, 0, -1))
    left((OWNO, 0, 0), (GQ, 0, -1))
    left((EXO, 3, 0))
    send((DO, 0, 1), (DO, 0, -1))
    came((EXQ, 2, 0))
    send((GQ, 2, 1), (GQ, 2, -1))
    left((OWNQ, 0, 0))
    left((GQ, 1, 1))
    came((EXQ, 3, 0))
    send((GQ, 3, 1), (GQ, 3, -1))
    send((DQ, 1, 2))
    left((EXQ, 3, 0))
    left((DQ, 0, -1))
    send((DQ, 1, -1))
    came((GQ, 0, 1))
    send((HQ, 0, 1))
    left((GQ, 1, -1))
    came((GQ, 2, 1), (GQ, 2, -1))
    send((HQ, 2, 1), (HQ, 2, -1))
    send((DQ, 1, 3))
    send((GO, 0, 1), (GO, 0, -1))
    left((DO, 0, 1), (DO, 0, -1))
    send((DO, 1, 1), (DO, 1, -1))
    left((GQ, 2, -1))
    came((DQ, 1, 2))
    send((RQ, 0, 0))
    left((GQ, 2, 1))
    came((GQ, 1, -1))
    send((HQ, 1, -1))
    came((DQ, 0, -1))
    send((RQ, 1, 0))
    came((DQ, 0, 1))
    send((AQ, 0, 1), (AQ, 0, 2))
    left((DQ, 0, 1), (GQ, 3, -1), (DQ, 1, 2))
    came((DQ, 1, 3))
    send((RQ, 0, 1), (AQ, 1, 1))
    came((DO, 0, 1), (DO, 0, -1))
    send((RO, 0, 1), (RO, 0, -1), (AO, 0, 0))
    came((EXO, 1, 0))
    send((GO, 1, 1), (GO, 1, -1))
    left((HQ, 2, -1), (DQ, 1, 3))
    came((GQ, 3, 1), (GQ, 3, -1))
    send((HQ, 3, 1), (HQ, 3, -1))
    left((GQ, 3, 1), (DO, 1, 1), (DO, 1, -1), (AQ, 0, 1), (AQ, 0, 2))
    came((RQ, 0, 0))
    send((AQ, 0, 4))
    came((DO, 1, 1), (DO, 1, -1))
    send((RO, 1, 1), (RO, 1, -1), (AO, 1, 0))
    left((HQ, 2, 1), (GO, 0, -1), (RQ, 0, 0), (AQ, 1, 1))
    left((DQ, 1, -1), (RQ, 1, 0))
    send((DQ, 2, -1))
    left((RQ, 0, 1))
    send((RQ, 3, 1))
    left((AO, 0, 0))
    came((RQ, 0, 1))
    send((AQ, 0, 5))
    came((EXO, 2, 0))
    send((GO, 2, 1), (GO, 2, -1))
    came((DQ, 1, -1))
    send((RQ, 2, 0))
    left((HQ, 0, 1), (GO, 0, 1), (RO, 0, 1), (RO, 0, -1))
    left((RQ, 3, 1))
    send((DQ, 2, 1))
    send((RQ, 3, 2))
    send((AQ, 1, 2))
    came((RQ, 1, 0))
    send((AQ, 1, 3))
    came((EXO, 3, 0))
    send((GO, 3, 1), (GO, 3, -1))
    left((HQ, 1, -1), (HQ, 3, 1), (HQ, 3, -1), (AQ, 0, 4), (AO, 1, 0), (AQ, 0, 5))
    came((GQ, 0, -1), (HQ, 0, 1), (GQ, 1, 1), (HQ, 1, -1), (HQ, 2, 1), (HQ, 2, -1), (HQ, 3, 1), (HQ, 3, -1))
    came((AQ, 0, 1), (AQ, 0, 2), (AQ, 0, 4), (AQ, 0, 5), (OWNQ, 0, 0))
    multiply_q(0)
    send((PQ, 0, 1), (PQ, 0, -1))
    left((GO, 1, -1), (RO, 1, 1), (RO, 1, -1))
    came((AQ, 1, 1), (AQ, 1, 2), (AQ, 1, 3))
    multiply_q(1)
    send((PQ, 1, 1), (PQ, 1, -1))
    left((GO, 1, 1))
    came((GO, 0, 1))
    send((HO, 0, 1))
    left((GO, 2, 1))
    came((GO, 1, -1))
    send((HO, 1, -1))
    came((RO, 0, 1), (RO, 0, -1))
    send((AO, 2, 0))
    came((RO, 1, 1), (RO, 1, -1))
    send((AO, 3, 0))
    left((AQ, 1, 2), (AQ, 1, 3))
    left((PQ, 0, 1))
    send((IQ, 0, 1), (IQ, 0, -1))
    left((GO, 2, -1), (GO, 3, -1))
    left((DQ, 2, -1))
    send((DQ, 3, -1))
    came((GO, 3, 1), (GO, 3, -1))
    send((HO, 3, 1), (HO, 3, -1))
    left((DQ, 2, 1))
    send((DQ, 3, 1))
    left((GO, 3, 1))
    came((GO, 2, 1), (GO, 2, -1))
    send((HO, 2, 1), (HO, 2, -1))
    left((RQ, 3, 2), (PQ, 0, -1), (AO, 2, 0), (AO, 3, 0))
    came((OWNO, 0, 0), (AO, 0, 0), (AO, 1, 0), (AO, 2, 0), (AO, 3, 0), (GO, 0, -1), (HO, 0, 1), (GO, 1, 1))
    came((HO, 1, -1))
    multiply_o(True)
    came((DQ, 2, 1), (DQ, 2, -1), (RQ, 2, 0))
    send((AQ, 2, 0))
    send((IQ, 1, 1), (IQ, 1, -1))
    came((HO, 2, 1), (HO, 2, -1), (HO, 3, 1), (HO, 3, -1))
    multiply_o(False)
    came((PQ, 1, 1), (PQ, 1, -1))
    join_q(1)
    send((LQ, 1, 1), (LQ, 1, -1))
    send((PO, 3, 1), (PO, 3, -1))
    send((IO, 3, 1), (IO, 3, -1))
    left((RQ, 2, 0), (PQ, 1, 1), (PQ, 1, -1), (HO, 0, 1), (HO, 1, -1), (IQ, 0, 1), (IQ, 0, -1), (HO, 3, 1))
    left((HO, 3, -1), (HO, 2, 1), (HO, 2, -1))
    came((AQ, 2, 0))
    multiply_q(2)
    send((PQ, 2, 1), (PQ, 2, -1))
    send((PO, 0, 1), (PO, 0, -1))
    came((DQ, 3, 1), (DQ, 3, -1), (RQ, 3, 1), (RQ, 3, 2))
    send((AQ, 3, 0))
    came((PQ, 0, 1), (PQ, 0, -1))
    join_q(0)
    send((LQ, 0, 1), (LQ, 0, -1))
    send((PO, 2, 1), (PO, 2, -1))
    left((DQ, 3, -1), (DQ, 3, 1), (AQ, 2, 0), (IQ, 1, 1), (IQ, 1, -1))
    came((PO, 3, 1), (PO, 3, -1))
    join_o(3)
    send((LO, 3, 1), (LO, 3, -1))
    left((PO, 3, 1), (PO, 3, -1), (IO, 3, 1), (IO, 3, -1))
    came((AQ, 3, 0))
    multiply_q(3)
    send((PQ, 3, 1), (PQ, 3, -1))
    left((PO, 0, 1))
    send((PO, 1, 1), (PO, 1, -1))
    came((IQ, 1, 1), (IQ, 1, -1), (LQ, 1, 1), (LQ, 1, -1))
    finish_q(1)
    send((FQ, 1, 0))
    send((IQ, 2, 1), (IQ, 2, -1))
    send((IO, 2, 1), (IO, 2, -1))
    left((LQ, 1, 1), (LQ, 1, -1), (PO, 0, -1), (AQ, 3, 0), (PO, 2, 1), (PO, 2, -1))
    came((IO, 3, 1), (IO, 3, -1), (LO, 3, 1), (LO, 3, -1))
    finish_o(3)
    came((PO, 0, 1), (PO, 0, -1))
    join_o(0)
    send((LO, 0, 1), (LO, 0, -1))
    left((LO, 3, 1), (LO, 3, -1))
    came((PQ, 2, 1), (PQ, 2, -1))
    join_q(2)
    send((LQ, 2, 1), (LQ, 2, -1))
    send((IO, 0, 1), (IO, 0, -1))
    send((IQ, 3, 1), (IQ, 3, -1))
    left((PQ, 2, 1), (PQ, 2, -1), (LQ, 0, 1), (LQ, 0, -1))
    left((PO, 1, 1))
    send((IO, 1, 1), (IO, 1, -1))
    came((PO, 1, 1), (PO, 1, -1))
    join_o(1)
    send((LO, 1, 1), (LO, 1, -1))
    left((PO, 1, -1), (IO, 2, 1), (IO, 2, -1))
    came((PQ, 3, 1), (PQ, 3, -1))
    join_q(3)
    send((LQ, 3, 1), (LQ, 3, -1))
    came((PO, 2, 1), (PO, 2, -1))
    join_o(2)
    send((LO, 2, 1), (LO, 2, -1))
    left((PQ, 3, 1), (PQ, 3, -1), (IQ, 2, 1), (IQ, 2, -1), (LO, 0, 1), (LO, 0, -1))
    came((IQ, 2, 1), (IQ, 2, -1), (LQ, 2, 1), (LQ, 2, -1))
    finish_q(2)
    send((FQ, 2, 0))
    came((IQ, 0, 1), (IQ, 0, -1), (LQ, 0, 1), (LQ, 0, -1))
    finish_q(0)
    send((FQ, 0, 0))
    came((IO, 0, 1), (IO, 0, -1), (LO, 0, 1), (LO, 0, -1))
    finish_o(0)
    send((FO, 0, 0))
    left((LQ, 2, 1), (LQ, 2, -1), (IO, 0, 1), (IO, 0, -1), (IQ, 3, 1), (IQ, 3, -1), (IO, 1, 1), (IO, 1, -1))
    left((LO, 1, 1), (LO, 1, -1), (LO, 2, 1), (LO, 2, -1))
    came((IO, 2, 1), (IO, 2, -1), (LO, 2, 1), (LO, 2, -1))
    finish_o(2)
    send((FO, 2, 0))
    came((IQ, 3, 1), (IQ, 3, -1), (LQ, 3, 1), (LQ, 3, -1))
    finish_q(3)
    came((IO, 1, 1), (IO, 1, -1), (LO, 1, 1), (LO, 1, -1))
    finish_o(1)
    send((FO, 1, 0))

    came(*list(open_came))
    left(*list(open_left))
    assert len(arrivals) == N_COME and len(locals_) == 7, len(arrivals)


def store(q_ref, o_ref, out_q, out_o, sem):
    copies = [pltpu.make_async_copy(q_ref, out_q, sem.at[0]), pltpu.make_async_copy(o_ref, out_o, sem.at[1])]
    for copy in copies:
        copy.start()
    for copy in copies:
        copy.wait()


def per_device(normed, qkv_grad, attn_out, out_grad):
    flat = [v.reshape(v.shape[0] * v.shape[1], v.shape[2]) for v in (normed, qkv_grad, attn_out, out_grad)]
    hbm = pl.BlockSpec(memory_space=pltpu.HBM)
    vmem = pl.BlockSpec(memory_space=pltpu.VMEM)
    out_q, out_o = pl.pallas_call(
        kernel,
        out_shape=(
            jax.ShapeDtypeStruct((2304, 128), F32),
            jax.ShapeDtypeStruct((72, 2048), F32),
        ),
        in_specs=[hbm] * 4,
        out_specs=[vmem] * 2,
        scratch_shapes=[
            pltpu.VMEM((128, 2304), BF16),
            pltpu.VMEM((2304, 128), BF16),
            pltpu.VMEM((576, 2048), BF16),
            pltpu.VMEM((4, 512, 2048), BF16),
            pltpu.VMEM((4, 4, 2, 288, 128), F32),
            pltpu.VMEM((4, 2, 288, 128), F32),
            pltpu.VMEM((4, 2, 2, 288, 128), F32),
            pltpu.VMEM((3, 576, 128), F32),
            pltpu.VMEM((3, 128, 512), BF16),
            pltpu.VMEM((4, 4, 128, 512), BF16),
            pltpu.VMEM((256, 1152), BF16),
            pltpu.VMEM((4, 288, 2048), BF16),
            pltpu.VMEM((4, 4, 2, 72, 256), F32),
            pltpu.VMEM((4, 2, 72, 256), F32),
            pltpu.VMEM((4, 2, 2, 72, 256), F32),
            pltpu.VMEM((3, 72, 512), F32),
            pltpu.SemaphoreType.DMA((N_SEND,)),
            pltpu.SemaphoreType.DMA((N_COME,)),
            pltpu.SemaphoreType.DMA((7,)),
        ],
        compiler_params=pltpu.CompilerParams(
            collective_id=0, has_side_effects=True, vmem_limit_bytes=40 * 1024 * 1024
        ),
        name="weight_grads",
    )(*[pltpu.with_memory_space_constraint(v, pltpu.HBM) for v in flat])
    out_q, out_o = pl.pallas_call(
        store,
        out_shape=(
            jax.ShapeDtypeStruct((2304, 128), F32),
            jax.ShapeDtypeStruct((72, 2048), F32),
        ),
        in_specs=[vmem] * 2,
        out_specs=[hbm] * 2,
        scratch_shapes=[pltpu.SemaphoreType.DMA((2,))],
        compiler_params=pltpu.CompilerParams(vmem_limit_bytes=1024 * 1024),
        name="store",
    )(out_q, out_o)
    return out_q, out_o.T


def solution(mesh):
    in_specs = (
        P("col", "depth", "row"),
        P("row", "depth", "col"),
        P("col", "depth", "row"),
        P("row", "depth", "col"),
    )
    out_specs = (P("row", ("col", "depth")), P("row", ("col", "depth")))
    return jax.shard_map(
        per_device, mesh=mesh, in_specs=in_specs, out_specs=out_specs, check_vma=False
    )
```

```python
import jax
import jax.numpy as jnp
from jax import lax
from jax.experimental import pallas as pl
from jax.experimental.pallas import tpu as pltpu
from jax.sharding import PartitionSpec as P

MESH = pl.DeviceIdType.MESH
F32 = jnp.float32
BF16 = jnp.bfloat16

(EXQ, EXO, GQ, GO, HQ, HO, OWNQ, OWNO, DQ, DO, RQ, RO, AQ, AO, PQ, PO, IQ, IO, LQ, LO, FQ, FO) = range(22)
STEP = {1: 1, 2: -1, 3: 2}
N_SEND, N_COME = 24, 69


def kernel(
    a_q, b_q, a_o, b_o, out_q, out_o,
    la_q, ta_q, at_q, vb_q, c_q, r1_q, r2_q, f_q,
    sa_o, va_o, lb_o, bt_o, c_o, r1_o, r2_o, f_o,
    ssem, rsem, lsem,
):
    row, x, depth = lax.axis_index("row"), lax.axis_index("col"), lax.axis_index("depth")
    z, y = depth // 4, depth % 4

    def at(dx=0, dy=0, dz=0):
        return (row, (x + dx + 4) % 4, ((z + dz + 4) % 4) * 4 + (y + dy + 4) % 4)

    def on(axis, step):
        return at(**{"d" + axis: step})

    sibling = (1 - row, x, depth)

    barrier = pltpu.get_barrier_semaphore()
    peers = [sibling, at(dx=1), at(dx=-1)]
    for axis in "yz":
        peers += [on(axis, 1), on(axis, -1), on(axis, 2)]
    for peer in peers:
        pl.semaphore_signal(barrier, inc=1, device_id=peer, device_id_type=MESH)

    locals_ = []

    def local(src, dst):
        copy = pltpu.make_async_copy(src, dst, lsem.at[len(locals_)])
        copy.start()
        locals_.append(copy)
        return copy

    def lanes(start, size=128):
        return pl.ds(pl.multiple_of(start, 128), size)

    mine = lanes(row * 256, 256)
    load_la_q = local(a_q, la_q)
    load_lb_o = local(b_o, lb_o)
    loads = [local(b_q, vb_q.at[0, mine, :])]
    for d in (1, 2, 3):
        to = (y + STEP[d] + 4) % 4
        loads.append(local(a_o.at[:, lanes(to * 512, 512)], sa_o.at[d - 1]))
    loads.append(local(a_o.at[:, lanes(y * 512, 512)], va_o.at[0, x]))

    def features(u):
        return pl.ds(pl.multiple_of((u + 4) % 4 * 576, 64), 576)

    load_la_q.wait()
    ta_q[...] = la_q[...].T
    for copy in loads:
        copy.wait()
    pl.semaphore_wait(barrier, len(peers))

    flows = {}

    def flow(kind, number, which, *pieces):
        flows[kind, number, which] = pieces

    ahead, behind = (x + 1) % 4, (x + 3) % 4

    def piece_q(s, c):
        return at_q.at[:, lanes(s * 512 + c * 128)]

    for d in (1, 2, 3):
        flow(EXQ, d, 0, (ta_q.at[features(z + STEP[d]), :], piece_q(d, x), on("z", STEP[d])))
        flow(EXO, d, 0, (sa_o.at[d - 1], va_o.at[d, x], on("y", STEP[d])))
    for s in range(4):
        for step in (1, -1):
            src = ta_q.at[features(z), :] if s == 0 else piece_q(s, x)
            flow(GQ, s, step, (src, piece_q(s, x), at(dx=step)))
            flow(GO, s, step, (va_o.at[s, x], va_o.at[s, x], at(dx=step)))
            came_from = behind if step == 1 else ahead
            if s < 2:
                part_q, part_o = piece_q(s, came_from), va_o.at[s, came_from]
            else:
                half = slice(0, 288) if step == 1 else slice(288, 576)
                part_q = at_q.at[half, lanes(s * 512 + came_from * 128)]
                half = slice(0, 64) if step == 1 else slice(64, 128)
                part_o = va_o.at[s, came_from, half]
            flow(HQ, s, step, (part_q, part_q, at(dx=step)))
            flow(HO, s, step, (part_o, part_o, at(dx=step)))

    order_q = [(z + 1 + s) % 4 for s in range(4)]
    halves = [lanes(row * 256 + h * 128, 128) for h in (0, 1)]

    def strip(d, rows, j):
        return vb_q.at[d, rows, lanes((j + 4) % 4 * 512, 512)]

    def same(part, device):
        return (part, part, device)

    for p in range(4):
        flow(DQ, p, 1, (strip(0, mine, z + 2 + p), strip(1, mine, z + 2 + p), at(dz=1)))
        flow(DQ, p, -1, (strip(0, mine, z + p), strip(2, mine, z + p), at(dz=-1)))
        for d in (1, 2, 3):
            flow(AQ, p, d, same(strip(d, mine, order_q[p]), sibling))
        flow(AQ, p, 0, *[same(strip(d, mine, order_q[p]), sibling) for d in (1, 2, 3)])
    for h in (0, 1):
        flow(DQ, 1, h + 2, (strip(0, halves[h], z + 3), strip(1, halves[h], z + 3), at(dz=1)))
        flow(RQ, 0, h, (strip(1, halves[h], z + 2), strip(3, halves[h], z + 2), at(dz=1)))
        flow(AQ, 0, h + 4, same(strip(3, halves[h], order_q[0]), sibling))
    flow(RQ, 3, 1, (strip(1, halves[0], z + 1), strip(3, halves[0], z + 1), at(dz=1)))
    flow(RQ, 3, 2, (strip(1, halves[1], z + 1), strip(3, halves[1], z + 1), at(dz=1)))
    flow(RQ, 1, 0, (strip(2, mine, z + 1), strip(3, mine, z + 1), at(dz=-1)))
    flow(RQ, 2, 0, (strip(2, mine, z + 2), strip(3, mine, z + 2), at(dz=-1)))
    flow(OWNQ, 0, 0, same(vb_q.at[0, mine, :], sibling))

    def turned(d, p, first=0, size=256):
        return bt_o.at[2 * p:2 * p + 2, :, lanes(d * 512 + row * 256 + first, size)]

    for p in (0, 1):
        for d in (1, 2):
            flow(DO, p, STEP[d], (turned(0, p), turned(d, p), at(dy=STEP[d])))
            first = (d - 1) * 128
            flow(RO, p, STEP[d], (turned(d, p, first, 128), turned(3, p, first, 128), at(dy=STEP[d])))
        flow(AO, p, 0, same(turned(1, p), sibling), same(turned(2, p), sibling))
        flow(AO, p + 2, 0, same(turned(3, p), sibling))
    own = bt_o.at[:, :, lanes(row * 256, 256)]
    flow(OWNO, 0, 0, same(own, sibling))

    order_o = [(y + 1 + s) % 4 for s in range(4)]

    def part_q(s, w, h):
        return c_q.at[order_q[s], (w + 4) % 4, h]

    def part_o(s, w, h):
        return c_o.at[(w + 4) % 4, order_o[s], h]

    for s in range(4):
        for axis, w, part, r1, r2, (far, near, late) in (
            ("y", y, part_q, r1_q, r2_q, (PQ, IQ, LQ)),
            ("z", z, part_o, r1_o, r2_o, (PO, IO, LO)),
        ):
            up, down = on(axis, 1), on(axis, -1)
            flow(far, s, 1, (part(s, w + 2, 0), r1.at[s, 0], up))
            flow(far, s, -1, (part(s, w + 2, 1), r1.at[s, 1], down))
            flow(near, s, 1, (part(s, w + 1, 1), r2.at[s, 0, 1], up))
            flow(near, s, -1, (part(s, w - 1, 0), r2.at[s, 1, 0], down))
            flow(late, s, 1, (part(s, w + 1, 0), r2.at[s, 0, 0], up))
            flow(late, s, -1, (part(s, w - 1, 1), r2.at[s, 1, 1], down))
    home_q = out_q.at[features(z), :]
    home_o = out_o.at[:, lanes(y * 512, 512)]
    for s in range(3):
        flow(FQ, s, 0, (f_q.at[s], home_q, (row, x, order_q[s] * 4 + y)))
        flow(FO, s, 0, (f_o.at[s], home_o, (row, x, z * 4 + order_o[s])))

    def multiply_q(s):
        j = order_q[s]

        @pl.loop(0, 2)
        def _(n):
            right = vb_q[:, :, lanes(j * 512 + n * 256, 256)].reshape(2048, 256)
            total = jnp.dot(at_q[...], right, preferred_element_type=F32)
            for c in (0, 1):
                for h in (0, 1):
                    c_q[j, 2 * n + c, h] = total[h * 288:(h + 1) * 288, c * 128:(c + 1) * 128]

    def multiply_o(first):
        slots, k = (slice(0, 2), slice(0, 1024)) if first else (slice(2, 4), slice(1024, 2048))

        @pl.loop(0, 4)
        def _(w):
            for h in (0, 1):
                right = va_o[slots, :, :, h * 256:(h + 1) * 256].reshape(1024, 256)
                total = jnp.dot(bt_o[w, :, k], right, preferred_element_type=F32)
                for j in range(4):
                    part = total[j * 72:(j + 1) * 72]
                    c_o[w, j, h] = part if first else c_o[w, j, h] + part

    def join(s, w, part, r1):
        for ref, k in ((part(s, w + 1, 0), 0), (part(s, w - 1, 1), 1)):
            ref[...] = ref[...] + r1[s, k]

    def join_q(s):
        join(s, y, part_q, r1_q)

    def join_o(s):
        join(s, z, part_o, r1_o)

    def finish_q(s):
        for h in (0, 1):
            rows = slice(h * 288, (h + 1) * 288)
            total = part_q(s, y, h)[...] + r2_q[s, 0, h] + r2_q[s, 1, h]
            if s < 3:
                f_q[s, rows] = total
            else:
                out_q[pl.ds(pl.multiple_of(z * 576 + h * 288, 32), 288)] = total

    def finish_o(s):
        for h in (0, 1):
            total = part_o(s, z, h)[...] + r2_o[s, 0, h] + r2_o[s, 1, h]
            if s < 3:
                f_o[s, :, h * 256:(h + 1) * 256] = total
            else:
                out_o[:, lanes(y * 512 + h * 256, 256)] = total

    whole = {}
    for s in range(4):
        for p, i, l, r1, r2 in ((PQ, IQ, LQ, r1_q, r2_q), (PO, IO, LO, r1_o, r2_o)):
            far, rest = r1.at[s], r2.at[s]
            for step in (1, -1):
                whole[p, s, step] = far
                whole[i, s, step] = whole[l, s, step] = rest
    for p in (2, 3):
        whole[AQ, p, 0] = vb_q.at[1:4, mine, lanes(order_q[p] * 512, 512)]
    together = at_q.at[:, 0:768]
    for name in ((GQ, 0, -1), (HQ, 0, 1), (GQ, 1, 1), (HQ, 1, -1), (HQ, 2, 1), (HQ, 2, -1), (HQ, 3, 1), (HQ, 3, -1)):
        whole[name] = together
    together = va_o.at[0]
    for name in ((GO, 0, -1), (HO, 0, 1), (GO, 1, 1), (HO, 1, -1)):
        whole[name] = together
    together = va_o.at[2, 0:2]
    for name in ((HO, 2, 1), (HO, 2, -1), (HO, 3, 1), (HO, 3, -1)):
        whole[name] = together
    together = bt_o.at[:, :, 0:1024]
    for name in ((OWNO, 0, 0), (AO, 0, 0), (AO, 1, 0), (AO, 2, 0), (AO, 3, 0)):
        whole[name] = together
    for p in (0, 1):
        two = bt_o.at[2 * p:2 * p + 2, :, 0:512]
        one = bt_o.at[2 * p:2 * p + 2, :, 0:256]
        for step in (1, -1):
            whole[DO, p, step], whole[RO, p, step] = two, one
    three_q, three_o = out_q.at[0:1728], out_o.at[:, 0:1536]
    for s in range(3):
        whole[FQ, s, 0], whole[FO, s, 0] = three_q, three_o
    copies, arrivals, free = {}, {}, list(range(N_SEND))
    open_left, open_came = {}, {}

    def send(*names):
        for name in names:
            copies[name] = []
            for src, dst, device in flows[name]:
                group = id(whole[name]) if name in whole else (name, len(copies[name]))
                arrival = arrivals.setdefault(group, len(arrivals))
                k = free.pop(0)
                copy = pltpu.make_async_remote_copy(
                    src, dst, ssem.at[k], rsem.at[arrival], device_id=device, device_id_type=MESH
                )
                copy.start()
                copies[name].append((copy, k))
            open_left[name] = open_came[name] = True

    def left(*names):
        for name in names:
            del open_left[name]
            for copy, k in copies[name]:
                copy.wait_send()
                free.append(k)

    def came(*names):
        for name in names:
            if name not in open_came:
                continue
            if name in whole:
                both = whole[name]
                arrival = arrivals[id(both)]
                pltpu.make_async_remote_copy(
                    both, both, ssem.at[0], rsem.at[arrival], device_id=sibling, device_id_type=MESH
                ).wait_recv()
                for other in whole:
                    if whole[other] is both:
                        open_came.pop(other, None)
            else:
                del open_came[name]
                for copy, _ in copies[name]:
                    copy.wait_recv()

    send((EXQ, 1, 0), (EXQ, 2, 0))
    send((GQ, 0, 1), (GQ, 0, -1))
    send((EXO, 1, 0), (EXO, 2, 0), (OWNQ, 0, 0))
    at_q[:, lanes(x * 128)] = ta_q[features(z), :]
    load_lb_o.wait()
    bt_o[:, :, lanes(row * 256, 256)] = lb_o[...].T.reshape(4, 288, 256)
    send((OWNO, 0, 0))
    left((EXO, 1, 0), (EXO, 2, 0))
    send((EXO, 3, 0))
    left((EXQ, 1, 0), (EXQ, 2, 0))
    send((EXQ, 3, 0))
    left((GQ, 0, 1))
    came((EXQ, 1, 0))
    send((GQ, 1, 1), (GQ, 1, -1))
    send((DQ, 0, 1), (DQ, 0, -1))
    left((OWNO, 0, 0), (GQ, 0, -1))
    left((EXO, 3, 0))
    send((DO, 0, 1), (DO, 0, -1))
    came((EXQ, 2, 0))
    send((GQ, 2, 1), (GQ, 2, -1))
    left((OWNQ, 0, 0))
    left((GQ, 1, 1))
    came((EXQ, 3, 0))
    send((GQ, 3, 1), (GQ, 3, -1))
    send((DQ, 1, 2))
    left((EXQ, 3, 0))
    left((DQ, 0, -1))
    send((DQ, 1, -1))
    came((GQ, 0, 1))
    send((HQ, 0, 1))
    left((GQ, 1, -1))
    came((GQ, 2, 1), (GQ, 2, -1))
    send((HQ, 2, 1), (HQ, 2, -1))
    send((DQ, 1, 3))
    send((GO, 0, 1), (GO, 0, -1))
    left((DO, 0, 1), (DO, 0, -1))
    send((DO, 1, 1), (DO, 1, -1))
    left((GQ, 2, -1))
    came((DQ, 1, 2))
    send((RQ, 0, 0))
    left((GQ, 2, 1))
    came((GQ, 1, -1))
    send((HQ, 1, -1))
    came((DQ, 0, -1))
    send((RQ, 1, 0))
    came((DQ, 0, 1))
    send((AQ, 0, 1), (AQ, 0, 2))
    left((DQ, 0, 1), (GQ, 3, -1), (DQ, 1, 2))
    came((DQ, 1, 3))
    send((RQ, 0, 1), (AQ, 1, 1))
    came((DO, 0, 1), (DO, 0, -1))
    send((RO, 0, 1), (RO, 0, -1), (AO, 0, 0))
    came((EXO, 1, 0))
    send((GO, 1, 1), (GO, 1, -1))
    left((HQ, 2, -1), (DQ, 1, 3))
    came((GQ, 3, 1), (GQ, 3, -1))
    send((HQ, 3, 1), (HQ, 3, -1))
    left((GQ, 3, 1), (DO, 1, 1), (DO, 1, -1), (AQ, 0, 1), (AQ, 0, 2))
    came((RQ, 0, 0))
    send((AQ, 0, 4))
    came((DO, 1, 1), (DO, 1, -1))
    send((RO, 1, 1), (RO, 1, -1), (AO, 1, 0))
    left((HQ, 2, 1), (GO, 0, -1), (RQ, 0, 0), (AQ, 1, 1))
    left((DQ, 1, -1), (RQ, 1, 0))
    send((DQ, 2, -1))
    left((RQ, 0, 1))
    send((RQ, 3, 1))
    left((AO, 0, 0))
    came((RQ, 0, 1))
    send((AQ, 0, 5))
    came((EXO, 2, 0))
    send((GO, 2, 1), (GO, 2, -1))
    came((DQ, 1, -1))
    send((RQ, 2, 0))
    left((HQ, 0, 1), (GO, 0, 1), (RO, 0, 1), (RO, 0, -1))
    left((RQ, 3, 1))
    send((DQ, 2, 1))
    send((RQ, 3, 2))
    send((AQ, 1, 2))
    came((RQ, 1, 0))
    send((AQ, 1, 3))
    came((EXO, 3, 0))
    send((GO, 3, 1), (GO, 3, -1))
    left((HQ, 1, -1), (HQ, 3, 1), (HQ, 3, -1), (AQ, 0, 4), (AO, 1, 0), (AQ, 0, 5))
    came((GQ, 0, -1), (HQ, 0, 1), (GQ, 1, 1), (HQ, 1, -1), (HQ, 2, 1), (HQ, 2, -1), (HQ, 3, 1), (HQ, 3, -1))
    came((AQ, 0, 1), (AQ, 0, 2), (AQ, 0, 4), (AQ, 0, 5), (OWNQ, 0, 0))
    multiply_q(0)
    send((PQ, 0, 1), (PQ, 0, -1))
    left((GO, 1, -1), (RO, 1, 1), (RO, 1, -1))
    came((AQ, 1, 1), (AQ, 1, 2), (AQ, 1, 3))
    multiply_q(1)
    send((PQ, 1, 1), (PQ, 1, -1))
    left((GO, 1, 1))
    came((GO, 0, 1))
    send((HO, 0, 1))
    left((GO, 2, 1))
    came((GO, 1, -1))
    send((HO, 1, -1))
    came((RO, 0, 1), (RO, 0, -1))
    send((AO, 2, 0))
    came((RO, 1, 1), (RO, 1, -1))
    send((AO, 3, 0))
    left((AQ, 1, 2), (AQ, 1, 3))
    left((PQ, 0, 1))
    send((IQ, 0, 1), (IQ, 0, -1))
    left((GO, 2, -1), (GO, 3, -1))
    left((DQ, 2, -1))
    send((DQ, 3, -1))
    came((GO, 3, 1), (GO, 3, -1))
    send((HO, 3, 1), (HO, 3, -1))
    left((DQ, 2, 1))
    send((DQ, 3, 1))
    left((GO, 3, 1))
    came((GO, 2, 1), (GO, 2, -1))
    send((HO, 2, 1), (HO, 2, -1))
    left((RQ, 3, 2), (PQ, 0, -1), (AO, 2, 0), (AO, 3, 0))
    came((OWNO, 0, 0), (AO, 0, 0), (AO, 1, 0), (AO, 2, 0), (AO, 3, 0), (GO, 0, -1), (HO, 0, 1), (GO, 1, 1))
    came((HO, 1, -1))
    multiply_o(True)
    came((DQ, 2, 1), (DQ, 2, -1), (RQ, 2, 0))
    send((AQ, 2, 0))
    send((IQ, 1, 1), (IQ, 1, -1))
    came((HO, 2, 1), (HO, 2, -1), (HO, 3, 1), (HO, 3, -1))
    multiply_o(False)
    came((PQ, 1, 1), (PQ, 1, -1))
    join_q(1)
    send((LQ, 1, 1), (LQ, 1, -1))
    send((PO, 3, 1), (PO, 3, -1))
    send((IO, 3, 1), (IO, 3, -1))
    left((RQ, 2, 0), (PQ, 1, 1), (PQ, 1, -1), (HO, 0, 1), (HO, 1, -1), (IQ, 0, 1), (IQ, 0, -1), (HO, 3, 1))
    left((HO, 3, -1), (HO, 2, 1), (HO, 2, -1))
    came((AQ, 2, 0))
    multiply_q(2)
    send((PQ, 2, 1), (PQ, 2, -1))
    send((PO, 0, 1), (PO, 0, -1))
    came((DQ, 3, 1), (DQ, 3, -1), (RQ, 3, 1), (RQ, 3, 2))
    send((AQ, 3, 0))
    came((PQ, 0, 1), (PQ, 0, -1))
    join_q(0)
    send((LQ, 0, 1), (LQ, 0, -1))
    send((PO, 2, 1), (PO, 2, -1))
    left((DQ, 3, -1), (DQ, 3, 1), (AQ, 2, 0), (IQ, 1, 1), (IQ, 1, -1))
    came((PO, 3, 1), (PO, 3, -1))
    join_o(3)
    send((LO, 3, 1), (LO, 3, -1))
    left((PO, 3, 1), (PO, 3, -1), (IO, 3, 1), (IO, 3, -1))
    came((AQ, 3, 0))
    multiply_q(3)
    send((PQ, 3, 1), (PQ, 3, -1))
    left((PO, 0, 1))
    send((PO, 1, 1), (PO, 1, -1))
    came((IQ, 1, 1), (IQ, 1, -1), (LQ, 1, 1), (LQ, 1, -1))
    finish_q(1)
    send((FQ, 1, 0))
    send((IQ, 2, 1), (IQ, 2, -1))
    send((IO, 2, 1), (IO, 2, -1))
    left((LQ, 1, 1), (LQ, 1, -1), (PO, 0, -1), (AQ, 3, 0), (PO, 2, 1), (PO, 2, -1))
    came((IO, 3, 1), (IO, 3, -1), (LO, 3, 1), (LO, 3, -1))
    finish_o(3)
    came((PO, 0, 1), (PO, 0, -1))
    join_o(0)
    send((LO, 0, 1), (LO, 0, -1))
    left((LO, 3, 1), (LO, 3, -1))
    came((PQ, 2, 1), (PQ, 2, -1))
    join_q(2)
    send((LQ, 2, 1), (LQ, 2, -1))
    send((IO, 0, 1), (IO, 0, -1))
    send((IQ, 3, 1), (IQ, 3, -1))
    left((PQ, 2, 1), (PQ, 2, -1), (LQ, 0, 1), (LQ, 0, -1))
    left((PO, 1, 1))
    send((IO, 1, 1), (IO, 1, -1))
    came((PO, 1, 1), (PO, 1, -1))
    join_o(1)
    send((LO, 1, 1), (LO, 1, -1))
    left((PO, 1, -1), (IO, 2, 1), (IO, 2, -1))
    came((PQ, 3, 1), (PQ, 3, -1))
    join_q(3)
    send((LQ, 3, 1), (LQ, 3, -1))
    came((PO, 2, 1), (PO, 2, -1))
    join_o(2)
    send((LO, 2, 1), (LO, 2, -1))
    left((PQ, 3, 1), (PQ, 3, -1), (IQ, 2, 1), (IQ, 2, -1), (LO, 0, 1), (LO, 0, -1))
    came((IQ, 2, 1), (IQ, 2, -1), (LQ, 2, 1), (LQ, 2, -1))
    finish_q(2)
    send((FQ, 2, 0))
    came((IQ, 0, 1), (IQ, 0, -1), (LQ, 0, 1), (LQ, 0, -1))
    finish_q(0)
    send((FQ, 0, 0))
    came((IO, 0, 1), (IO, 0, -1), (LO, 0, 1), (LO, 0, -1))
    finish_o(0)
    send((FO, 0, 0))
    left((LQ, 2, 1), (LQ, 2, -1), (IO, 0, 1), (IO, 0, -1), (IQ, 3, 1), (IQ, 3, -1), (IO, 1, 1), (IO, 1, -1))
    left((LO, 1, 1), (LO, 1, -1), (LO, 2, 1), (LO, 2, -1))
    came((IO, 2, 1), (IO, 2, -1), (LO, 2, 1), (LO, 2, -1))
    finish_o(2)
    send((FO, 2, 0))
    came((IQ, 3, 1), (IQ, 3, -1), (LQ, 3, 1), (LQ, 3, -1))
    finish_q(3)
    came((IO, 1, 1), (IO, 1, -1), (LO, 1, 1), (LO, 1, -1))
    finish_o(1)
    send((FO, 1, 0))

    came(*list(open_came))
    left(*list(open_left))
    assert len(arrivals) == N_COME and len(locals_) == 7, len(arrivals)


def store(q_ref, o_ref, out_q, out_o, sem):
    copies = [pltpu.make_async_copy(q_ref, out_q, sem.at[0]), pltpu.make_async_copy(o_ref, out_o, sem.at[1])]
    for copy in copies:
        copy.start()
    for copy in copies:
        copy.wait()


def per_device(normed, qkv_grad, attn_out, out_grad):
    flat = [v.reshape(v.shape[0] * v.shape[1], v.shape[2]) for v in (normed, qkv_grad, attn_out, out_grad)]
    hbm = pl.BlockSpec(memory_space=pltpu.HBM)
    vmem = pl.BlockSpec(memory_space=pltpu.VMEM)
    out_q, out_o = pl.pallas_call(
        kernel,
        out_shape=(
            jax.ShapeDtypeStruct((2304, 128), F32),
            jax.ShapeDtypeStruct((72, 2048), F32),
        ),
        in_specs=[hbm] * 4,
        out_specs=[vmem] * 2,
        scratch_shapes=[
            pltpu.VMEM((128, 2304), BF16),
            pltpu.VMEM((2304, 128), BF16),
            pltpu.VMEM((576, 2048), BF16),
            pltpu.VMEM((4, 512, 2048), BF16),
            pltpu.VMEM((4, 4, 2, 288, 128), F32),
            pltpu.VMEM((4, 2, 288, 128), F32),
            pltpu.VMEM((4, 2, 2, 288, 128), F32),
            pltpu.VMEM((3, 576, 128), F32),
            pltpu.VMEM((3, 128, 512), BF16),
            pltpu.VMEM((4, 4, 128, 512), BF16),
            pltpu.VMEM((256, 1152), BF16),
            pltpu.VMEM((4, 288, 2048), BF16),
            pltpu.VMEM((4, 4, 2, 72, 256), F32),
            pltpu.VMEM((4, 2, 72, 256), F32),
            pltpu.VMEM((4, 2, 2, 72, 256), F32),
            pltpu.VMEM((3, 72, 512), F32),
            pltpu.SemaphoreType.DMA((N_SEND,)),
            pltpu.SemaphoreType.DMA((N_COME,)),
            pltpu.SemaphoreType.DMA((7,)),
        ],
        compiler_params=pltpu.CompilerParams(
            collective_id=0, has_side_effects=True, vmem_limit_bytes=40 * 1024 * 1024
        ),
        name="weight_grads",
    )(*[pltpu.with_memory_space_constraint(v, pltpu.HBM) for v in flat])
    out_q, out_o = pl.pallas_call(
        store,
        out_shape=(
            jax.ShapeDtypeStruct((2304, 128), F32),
            jax.ShapeDtypeStruct((72, 2048), F32),
        ),
        in_specs=[vmem] * 2,
        out_specs=[hbm] * 2,
        scratch_shapes=[pltpu.SemaphoreType.DMA((2,))],
        compiler_params=pltpu.CompilerParams(vmem_limit_bytes=1024 * 1024),
        name="store",
    )(out_q, out_o)
    return out_q, out_o.T


def solution(mesh):
    in_specs = (
        P("col", "depth", "row"),
        P("row", "depth", "col"),
        P("col", "depth", "row"),
        P("row", "depth", "col"),
    )
    out_specs = (P("row", ("col", "depth")), P("row", ("col", "depth")))
    return jax.shard_map(
        per_device, mesh=mesh, in_specs=in_specs, out_specs=out_specs, check_vma=False
    )
```

```python
import jax
import jax.numpy as jnp
from jax import lax
from jax.experimental import pallas as pl
from jax.experimental.pallas import tpu as pltpu
from jax.sharding import PartitionSpec as P

MESH = pl.DeviceIdType.MESH
F32 = jnp.float32
BF16 = jnp.bfloat16

(EXQ, EXO, GQ, GO, HQ, HO, OWNQ, OWNO, DQ, DO, RQ, RO, AQ, AO, PQ, PO, IQ, IO, LQ, LO, FQ, FO) = range(22)
STEP = {1: 1, 2: -1, 3: 2}
N_SEND, N_COME = 24, 69


def kernel(
    a_q, b_q, a_o, b_o, out_q, out_o,
    la_q, ta_q, at_q, vb_q, c_q, r1_q, r2_q, f_q,
    sa_o, va_o, lb_o, bt_o, c_o, r1_o, r2_o, f_o,
    ssem, rsem, lsem,
):
    row, x, depth = lax.axis_index("row"), lax.axis_index("col"), lax.axis_index("depth")
    z, y = depth // 4, depth % 4

    def at(dx=0, dy=0, dz=0):
        return (row, (x + dx + 4) % 4, ((z + dz + 4) % 4) * 4 + (y + dy + 4) % 4)

    def on(axis, step):
        return at(**{"d" + axis: step})

    sibling = (1 - row, x, depth)

    barrier = pltpu.get_barrier_semaphore()
    peers = [sibling, at(dx=1), at(dx=-1)]
    for axis in "yz":
        peers += [on(axis, 1), on(axis, -1), on(axis, 2)]
    for peer in peers:
        pl.semaphore_signal(barrier, inc=1, device_id=peer, device_id_type=MESH)

    locals_ = []

    def local(src, dst):
        copy = pltpu.make_async_copy(src, dst, lsem.at[len(locals_)])
        copy.start()
        locals_.append(copy)
        return copy

    def lanes(start, size=128):
        return pl.ds(pl.multiple_of(start, 128), size)

    mine = lanes(row * 256, 256)
    load_la_q = local(a_q, la_q)
    load_lb_o = local(b_o, lb_o)
    loads = [local(b_q, vb_q.at[0, mine, :])]
    for d in (1, 2, 3):
        to = (y + STEP[d] + 4) % 4
        loads.append(local(a_o.at[:, lanes(to * 512, 512)], sa_o.at[d - 1]))
    loads.append(local(a_o.at[:, lanes(y * 512, 512)], va_o.at[0, x]))

    def features(u):
        return pl.ds(pl.multiple_of((u + 4) % 4 * 576, 64), 576)

    load_la_q.wait()
    ta_q[...] = la_q[...].T
    for copy in loads:
        copy.wait()
    pl.semaphore_wait(barrier, len(peers))

    flows = {}

    def flow(kind, number, which, *pieces):
        flows[kind, number, which] = pieces

    ahead, behind = (x + 1) % 4, (x + 3) % 4

    def piece_q(s, c):
        return at_q.at[:, lanes(s * 512 + c * 128)]

    for d in (1, 2, 3):
        flow(EXQ, d, 0, (ta_q.at[features(z + STEP[d]), :], piece_q(d, x), on("z", STEP[d])))
        flow(EXO, d, 0, (sa_o.at[d - 1], va_o.at[d, x], on("y", STEP[d])))
    for s in range(4):
        for step in (1, -1):
            src = ta_q.at[features(z), :] if s == 0 else piece_q(s, x)
            flow(GQ, s, step, (src, piece_q(s, x), at(dx=step)))
            flow(GO, s, step, (va_o.at[s, x], va_o.at[s, x], at(dx=step)))
            came_from = behind if step == 1 else ahead
            if s < 2:
                part_q, part_o = piece_q(s, came_from), va_o.at[s, came_from]
            else:
                half = slice(0, 288) if step == 1 else slice(288, 576)
                part_q = at_q.at[half, lanes(s * 512 + came_from * 128)]
                half = slice(0, 64) if step == 1 else slice(64, 128)
                part_o = va_o.at[s, came_from, half]
            flow(HQ, s, step, (part_q, part_q, at(dx=step)))
            flow(HO, s, step, (part_o, part_o, at(dx=step)))

    order_q = [(z + 1 + s) % 4 for s in range(4)]
    halves = [lanes(row * 256 + h * 128, 128) for h in (0, 1)]

    def strip(d, rows, j):
        return vb_q.at[d, rows, lanes((j + 4) % 4 * 512, 512)]

    def same(part, device):
        return (part, part, device)

    for p in range(4):
        flow(DQ, p, 1, (strip(0, mine, z + 2 + p), strip(1, mine, z + 2 + p), at(dz=1)))
        flow(DQ, p, -1, (strip(0, mine, z + p), strip(2, mine, z + p), at(dz=-1)))
        for d in (1, 2, 3):
            flow(AQ, p, d, same(strip(d, mine, order_q[p]), sibling))
        flow(AQ, p, 0, *[same(strip(d, mine, order_q[p]), sibling) for d in (1, 2, 3)])
    for h in (0, 1):
        flow(DQ, 1, h + 2, (strip(0, halves[h], z + 3), strip(1, halves[h], z + 3), at(dz=1)))
        flow(RQ, 0, h, (strip(1, halves[h], z + 2), strip(3, halves[h], z + 2), at(dz=1)))
        flow(AQ, 0, h + 4, same(strip(3, halves[h], order_q[0]), sibling))
    flow(RQ, 3, 1, (strip(1, halves[0], z + 1), strip(3, halves[0], z + 1), at(dz=1)))
    flow(RQ, 3, 2, (strip(1, halves[1], z + 1), strip(3, halves[1], z + 1), at(dz=1)))
    flow(RQ, 1, 0, (strip(2, mine, z + 1), strip(3, mine, z + 1), at(dz=-1)))
    flow(RQ, 2, 0, (strip(2, mine, z + 2), strip(3, mine, z + 2), at(dz=-1)))
    flow(OWNQ, 0, 0, same(vb_q.at[0, mine, :], sibling))

    def turned(d, p, first=0, size=256):
        return bt_o.at[2 * p:2 * p + 2, :, lanes(d * 512 + row * 256 + first, size)]

    for p in (0, 1):
        for d in (1, 2):
            flow(DO, p, STEP[d], (turned(0, p), turned(d, p), at(dy=STEP[d])))
            first = (d - 1) * 128
            flow(RO, p, STEP[d], (turned(d, p, first, 128), turned(3, p, first, 128), at(dy=STEP[d])))
        flow(AO, p, 0, same(turned(1, p), sibling), same(turned(2, p), sibling))
        flow(AO, p + 2, 0, same(turned(3, p), sibling))
    own = bt_o.at[:, :, lanes(row * 256, 256)]
    flow(OWNO, 0, 0, same(own, sibling))

    order_o = [(y + 1 + s) % 4 for s in range(4)]

    def part_q(s, w, h):
        return c_q.at[order_q[s], (w + 4) % 4, h]

    def part_o(s, w, h):
        return c_o.at[(w + 4) % 4, order_o[s], h]

    for s in range(4):
        for axis, w, part, r1, r2, (far, near, late) in (
            ("y", y, part_q, r1_q, r2_q, (PQ, IQ, LQ)),
            ("z", z, part_o, r1_o, r2_o, (PO, IO, LO)),
        ):
            up, down = on(axis, 1), on(axis, -1)
            flow(far, s, 1, (part(s, w + 2, 0), r1.at[s, 0], up))
            flow(far, s, -1, (part(s, w + 2, 1), r1.at[s, 1], down))
            flow(near, s, 1, (part(s, w + 1, 1), r2.at[s, 0, 1], up))
            flow(near, s, -1, (part(s, w - 1, 0), r2.at[s, 1, 0], down))
            flow(late, s, 1, (part(s, w + 1, 0), r2.at[s, 0, 0], up))
            flow(late, s, -1, (part(s, w - 1, 1), r2.at[s, 1, 1], down))
    home_q = out_q.at[features(z), :]
    home_o = out_o.at[:, lanes(y * 512, 512)]
    for s in range(3):
        flow(FQ, s, 0, (f_q.at[s], home_q, (row, x, order_q[s] * 4 + y)))
        flow(FO, s, 0, (f_o.at[s], home_o, (row, x, z * 4 + order_o[s])))

    def multiply_q(s):
        j = order_q[s]

        @pl.loop(0, 2)
        def _(n):
            right = vb_q[:, :, lanes(j * 512 + n * 256, 256)].reshape(2048, 256)
            total = jnp.dot(at_q[...], right, preferred_element_type=F32)
            for c in (0, 1):
                for h in (0, 1):
                    c_q[j, 2 * n + c, h] = total[h * 288:(h + 1) * 288, c * 128:(c + 1) * 128]

    def multiply_o(first):
        slots, k = (slice(0, 2), slice(0, 1024)) if first else (slice(2, 4), slice(1024, 2048))

        @pl.loop(0, 4)
        def _(w):
            for h in (0, 1):
                right = va_o[slots, :, :, h * 256:(h + 1) * 256].reshape(1024, 256)
                total = jnp.dot(bt_o[w, :, k], right, preferred_element_type=F32)
                for j in range(4):
                    part = total[j * 72:(j + 1) * 72]
                    c_o[w, j, h] = part if first else c_o[w, j, h] + part

    def join(s, w, part, r1):
        for ref, k in ((part(s, w + 1, 0), 0), (part(s, w - 1, 1), 1)):
            ref[...] = ref[...] + r1[s, k]

    def join_q(s):
        join(s, y, part_q, r1_q)

    def join_o(s):
        join(s, z, part_o, r1_o)

    def finish_q(s):
        for h in (0, 1):
            rows = slice(h * 288, (h + 1) * 288)
            total = part_q(s, y, h)[...] + r2_q[s, 0, h] + r2_q[s, 1, h]
            if s < 3:
                f_q[s, rows] = total
            else:
                out_q[pl.ds(pl.multiple_of(z * 576 + h * 288, 32), 288)] = total

    def finish_o(s):
        for h in (0, 1):
            total = part_o(s, z, h)[...] + r2_o[s, 0, h] + r2_o[s, 1, h]
            if s < 3:
                f_o[s, :, h * 256:(h + 1) * 256] = total
            else:
                out_o[:, lanes(y * 512 + h * 256, 256)] = total

    whole = {}
    for s in range(4):
        for p, i, l, r1, r2 in ((PQ, IQ, LQ, r1_q, r2_q), (PO, IO, LO, r1_o, r2_o)):
            far, rest = r1.at[s], r2.at[s]
            for step in (1, -1):
                whole[p, s, step] = far
                whole[i, s, step] = whole[l, s, step] = rest
    for p in (2, 3):
        whole[AQ, p, 0] = vb_q.at[1:4, mine, lanes(order_q[p] * 512, 512)]
    together = at_q.at[:, 0:768]
    for name in ((GQ, 0, -1), (HQ, 0, 1), (GQ, 1, 1), (HQ, 1, -1), (HQ, 2, 1), (HQ, 2, -1), (HQ, 3, 1), (HQ, 3, -1)):
        whole[name] = together
    together = va_o.at[0]
    for name in ((GO, 0, -1), (HO, 0, 1), (GO, 1, 1), (HO, 1, -1)):
        whole[name] = together
    together = va_o.at[2, 0:2]
    for name in ((HO, 2, 1), (HO, 2, -1), (HO, 3, 1), (HO, 3, -1)):
        whole[name] = together
    together = bt_o.at[:, :, 0:1024]
    for name in ((OWNO, 0, 0), (AO, 0, 0), (AO, 1, 0), (AO, 2, 0), (AO, 3, 0)):
        whole[name] = together
    for p in (0, 1):
        two = bt_o.at[2 * p:2 * p + 2, :, 0:512]
        one = bt_o.at[2 * p:2 * p + 2, :, 0:256]
        for step in (1, -1):
            whole[DO, p, step], whole[RO, p, step] = two, one
    three_q, three_o = out_q.at[0:1728], out_o.at[:, 0:1536]
    for s in range(3):
        whole[FQ, s, 0], whole[FO, s, 0] = three_q, three_o
    copies, arrivals, free = {}, {}, list(range(N_SEND))
    open_left, open_came = {}, {}

    def send(*names):
        for name in names:
            copies[name] = []
            for src, dst, device in flows[name]:
                group = id(whole[name]) if name in whole else (name, len(copies[name]))
                arrival = arrivals.setdefault(group, len(arrivals))
                k = free.pop(0)
                copy = pltpu.make_async_remote_copy(
                    src, dst, ssem.at[k], rsem.at[arrival], device_id=device, device_id_type=MESH
                )
                copy.start()
                copies[name].append((copy, k))
            open_left[name] = open_came[name] = True

    def left(*names):
        for name in names:
            del open_left[name]
            for copy, k in copies[name]:
                copy.wait_send()
                free.append(k)

    def came(*names):
        for name in names:
            if name not in open_came:
                continue
            if name in whole:
                both = whole[name]
                arrival = arrivals[id(both)]
                pltpu.make_async_remote_copy(
                    both, both, ssem.at[0], rsem.at[arrival], device_id=sibling, device_id_type=MESH
                ).wait_recv()
                for other in whole:
                    if whole[other] is both:
                        open_came.pop(other, None)
            else:
                del open_came[name]
                for copy, _ in copies[name]:
                    copy.wait_recv()

    send((EXQ, 1, 0), (EXQ, 2, 0))
    send((GQ, 0, 1), (GQ, 0, -1))
    send((EXO, 1, 0), (EXO, 2, 0), (OWNQ, 0, 0))
    at_q[:, lanes(x * 128)] = ta_q[features(z), :]
    load_lb_o.wait()
    bt_o[:, :, lanes(row * 256, 256)] = lb_o[...].T.reshape(4, 288, 256)
    send((OWNO, 0, 0))
    left((EXO, 1, 0), (EXO, 2, 0))
    send((EXO, 3, 0))
    left((EXQ, 1, 0), (EXQ, 2, 0))
    send((EXQ, 3, 0))
    left((GQ, 0, 1))
    came((EXQ, 1, 0))
    send((GQ, 1, 1), (GQ, 1, -1))
    send((DQ, 0, 1), (DQ, 0, -1))
    left((OWNO, 0, 0), (GQ, 0, -1))
    left((EXO, 3, 0))
    send((DO, 0, 1), (DO, 0, -1))
    came((EXQ, 2, 0))
    send((GQ, 2, 1), (GQ, 2, -1))
    left((OWNQ, 0, 0))
    left((GQ, 1, 1))
    came((EXQ, 3, 0))
    send((GQ, 3, 1), (GQ, 3, -1))
    send((DQ, 1, 2))
    left((EXQ, 3, 0))
    left((DQ, 0, -1))
    send((DQ, 1, -1))
    came((GQ, 0, 1))
    send((HQ, 0, 1))
    left((GQ, 1, -1))
    came((GQ, 2, 1), (GQ, 2, -1))
    send((HQ, 2, 1), (HQ, 2, -1))
    send((DQ, 1, 3))
    send((GO, 0, 1), (GO, 0, -1))
    left((DO, 0, 1), (DO, 0, -1))
    send((DO, 1, 1), (DO, 1, -1))
    left((GQ, 2, -1))
    came((DQ, 1, 2))
    send((RQ, 0, 0))
    left((GQ, 2, 1))
    came((GQ, 1, -1))
    send((HQ, 1, -1))
    came((DQ, 0, -1))
    send((RQ, 1, 0))
    came((DQ, 0, 1))
    send((AQ, 0, 1), (AQ, 0, 2))
    left((DQ, 0, 1), (GQ, 3, -1), (DQ, 1, 2))
    came((DQ, 1, 3))
    send((RQ, 0, 1), (AQ, 1, 1))
    came((DO, 0, 1), (DO, 0, -1))
    send((RO, 0, 1), (RO, 0, -1), (AO, 0, 0))
    came((EXO, 1, 0))
    send((GO, 1, 1), (GO, 1, -1))
    left((HQ, 2, -1), (DQ, 1, 3))
    came((GQ, 3, 1), (GQ, 3, -1))
    send((HQ, 3, 1), (HQ, 3, -1))
    left((GQ, 3, 1), (DO, 1, 1), (DO, 1, -1), (AQ, 0, 1), (AQ, 0, 2))
    came((RQ, 0, 0))
    send((AQ, 0, 4))
    came((DO, 1, 1), (DO, 1, -1))
    send((RO, 1, 1), (RO, 1, -1), (AO, 1, 0))
    left((HQ, 2, 1), (GO, 0, -1), (RQ, 0, 0), (AQ, 1, 1))
    left((DQ, 1, -1), (RQ, 1, 0))
    send((DQ, 2, -1))
    left((RQ, 0, 1))
    send((RQ, 3, 1))
    left((AO, 0, 0))
    came((RQ, 0, 1))
    send((AQ, 0, 5))
    came((EXO, 2, 0))
    send((GO, 2, 1), (GO, 2, -1))
    came((DQ, 1, -1))
    send((RQ, 2, 0))
    left((HQ, 0, 1), (GO, 0, 1), (RO, 0, 1), (RO, 0, -1))
    left((RQ, 3, 1))
    send((DQ, 2, 1))
    send((RQ, 3, 2))
    send((AQ, 1, 2))
    came((RQ, 1, 0))
    send((AQ, 1, 3))
    came((EXO, 3, 0))
    send((GO, 3, 1), (GO, 3, -1))
    left((HQ, 1, -1), (HQ, 3, 1), (HQ, 3, -1), (AQ, 0, 4), (AO, 1, 0), (AQ, 0, 5))
    came((GQ, 0, -1), (HQ, 0, 1), (GQ, 1, 1), (HQ, 1, -1), (HQ, 2, 1), (HQ, 2, -1), (HQ, 3, 1), (HQ, 3, -1))
    came((AQ, 0, 1), (AQ, 0, 2), (AQ, 0, 4), (AQ, 0, 5), (OWNQ, 0, 0))
    multiply_q(0)
    send((PQ, 0, 1), (PQ, 0, -1))
    left((GO, 1, -1), (RO, 1, 1), (RO, 1, -1))
    came((AQ, 1, 1), (AQ, 1, 2), (AQ, 1, 3))
    multiply_q(1)
    send((PQ, 1, 1), (PQ, 1, -1))
    left((GO, 1, 1))
    came((GO, 0, 1))
    send((HO, 0, 1))
    left((GO, 2, 1))
    came((GO, 1, -1))
    send((HO, 1, -1))
    came((RO, 0, 1), (RO, 0, -1))
    send((AO, 2, 0))
    came((RO, 1, 1), (RO, 1, -1))
    send((AO, 3, 0))
    left((AQ, 1, 2), (AQ, 1, 3))
    left((PQ, 0, 1))
    send((IQ, 0, 1), (IQ, 0, -1))
    left((GO, 2, -1), (GO, 3, -1))
    left((DQ, 2, -1))
    send((DQ, 3, -1))
    came((GO, 3, 1), (GO, 3, -1))
    send((HO, 3, 1), (HO, 3, -1))
    left((DQ, 2, 1))
    send((DQ, 3, 1))
    left((GO, 3, 1))
    came((GO, 2, 1), (GO, 2, -1))
    send((HO, 2, 1), (HO, 2, -1))
    left((RQ, 3, 2), (PQ, 0, -1), (AO, 2, 0), (AO, 3, 0))
    came((OWNO, 0, 0), (AO, 0, 0), (AO, 1, 0), (AO, 2, 0), (AO, 3, 0), (GO, 0, -1), (HO, 0, 1), (GO, 1, 1))
    came((HO, 1, -1))
    multiply_o(True)
    came((DQ, 2, 1), (DQ, 2, -1), (RQ, 2, 0))
    send((AQ, 2, 0))
    send((IQ, 1, 1), (IQ, 1, -1))
    came((HO, 2, 1), (HO, 2, -1), (HO, 3, 1), (HO, 3, -1))
    multiply_o(False)
    came((PQ, 1, 1), (PQ, 1, -1))
    join_q(1)
    send((LQ, 1, 1), (LQ, 1, -1))
    send((PO, 3, 1), (PO, 3, -1))
    send((IO, 3, 1), (IO, 3, -1))
    left((RQ, 2, 0), (PQ, 1, 1), (PQ, 1, -1), (HO, 0, 1), (HO, 1, -1), (IQ, 0, 1), (IQ, 0, -1), (HO, 3, 1))
    left((HO, 3, -1), (HO, 2, 1), (HO, 2, -1))
    came((AQ, 2, 0))
    multiply_q(2)
    send((PQ, 2, 1), (PQ, 2, -1))
    send((PO, 0, 1), (PO, 0, -1))
    came((DQ, 3, 1), (DQ, 3, -1), (RQ, 3, 1), (RQ, 3, 2))
    send((AQ, 3, 0))
    came((PQ, 0, 1), (PQ, 0, -1))
    join_q(0)
    send((LQ, 0, 1), (LQ, 0, -1))
    send((PO, 2, 1), (PO, 2, -1))
    left((DQ, 3, -1), (DQ, 3, 1), (AQ, 2, 0), (IQ, 1, 1), (IQ, 1, -1))
    came((PO, 3, 1), (PO, 3, -1))
    join_o(3)
    send((LO, 3, 1), (LO, 3, -1))
    left((PO, 3, 1), (PO, 3, -1), (IO, 3, 1), (IO, 3, -1))
    came((AQ, 3, 0))
    multiply_q(3)
    send((PQ, 3, 1), (PQ, 3, -1))
    left((PO, 0, 1))
    send((PO, 1, 1), (PO, 1, -1))
    came((IQ, 1, 1), (IQ, 1, -1), (LQ, 1, 1), (LQ, 1, -1))
    finish_q(1)
    send((FQ, 1, 0))
    send((IQ, 2, 1), (IQ, 2, -1))
    send((IO, 2, 1), (IO, 2, -1))
    left((LQ, 1, 1), (LQ, 1, -1), (PO, 0, -1), (AQ, 3, 0), (PO, 2, 1), (PO, 2, -1))
    came((IO, 3, 1), (IO, 3, -1), (LO, 3, 1), (LO, 3, -1))
    finish_o(3)
    came((PO, 0, 1), (PO, 0, -1))
    join_o(0)
    send((LO, 0, 1), (LO, 0, -1))
    left((LO, 3, 1), (LO, 3, -1))
    came((PQ, 2, 1), (PQ, 2, -1))
    join_q(2)
    send((LQ, 2, 1), (LQ, 2, -1))
    send((IO, 0, 1), (IO, 0, -1))
    send((IQ, 3, 1), (IQ, 3, -1))
    left((PQ, 2, 1), (PQ, 2, -1), (LQ, 0, 1), (LQ, 0, -1))
    left((PO, 1, 1))
    send((IO, 1, 1), (IO, 1, -1))
    came((PO, 1, 1), (PO, 1, -1))
    join_o(1)
    send((LO, 1, 1), (LO, 1, -1))
    left((PO, 1, -1), (IO, 2, 1), (IO, 2, -1))
    came((PQ, 3, 1), (PQ, 3, -1))
    join_q(3)
    send((LQ, 3, 1), (LQ, 3, -1))
    came((PO, 2, 1), (PO, 2, -1))
    join_o(2)
    send((LO, 2, 1), (LO, 2, -1))
    left((PQ, 3, 1), (PQ, 3, -1), (IQ, 2, 1), (IQ, 2, -1), (LO, 0, 1), (LO, 0, -1))
    came((IQ, 2, 1), (IQ, 2, -1), (LQ, 2, 1), (LQ, 2, -1))
    finish_q(2)
    send((FQ, 2, 0))
    came((IQ, 0, 1), (IQ, 0, -1), (LQ, 0, 1), (LQ, 0, -1))
    finish_q(0)
    send((FQ, 0, 0))
    came((IO, 0, 1), (IO, 0, -1), (LO, 0, 1), (LO, 0, -1))
    finish_o(0)
    send((FO, 0, 0))
    left((LQ, 2, 1), (LQ, 2, -1), (IO, 0, 1), (IO, 0, -1), (IQ, 3, 1), (IQ, 3, -1), (IO, 1, 1), (IO, 1, -1))
    left((LO, 1, 1), (LO, 1, -1), (LO, 2, 1), (LO, 2, -1))
    came((IO, 2, 1), (IO, 2, -1), (LO, 2, 1), (LO, 2, -1))
    finish_o(2)
    send((FO, 2, 0))
    came((IQ, 3, 1), (IQ, 3, -1), (LQ, 3, 1), (LQ, 3, -1))
    finish_q(3)
    came((IO, 1, 1), (IO, 1, -1), (LO, 1, 1), (LO, 1, -1))
    finish_o(1)
    send((FO, 1, 0))

    came(*list(open_came))
    left(*list(open_left))
    assert len(arrivals) == N_COME and len(locals_) == 7, len(arrivals)


def store(q_ref, o_ref, out_q, out_o, sem):
    copies = [pltpu.make_async_copy(o_ref, out_o, sem.at[4])]
    for k in range(4):
        rows = pl.ds(k * 576, 576)
        copies.append(pltpu.make_async_copy(q_ref.at[rows], out_q.at[rows], sem.at[k]))
    for copy in copies:
        copy.start()
    for copy in copies:
        copy.wait()


def per_device(normed, qkv_grad, attn_out, out_grad):
    flat = [v.reshape(v.shape[0] * v.shape[1], v.shape[2]) for v in (normed, qkv_grad, attn_out, out_grad)]
    hbm = pl.BlockSpec(memory_space=pltpu.HBM)
    vmem = pl.BlockSpec(memory_space=pltpu.VMEM)
    out_q, out_o = pl.pallas_call(
        kernel,
        out_shape=(
            jax.ShapeDtypeStruct((2304, 128), F32),
            jax.ShapeDtypeStruct((72, 2048), F32),
        ),
        in_specs=[hbm] * 4,
        out_specs=[vmem] * 2,
        scratch_shapes=[
            pltpu.VMEM((128, 2304), BF16),
            pltpu.VMEM((2304, 128), BF16),
            pltpu.VMEM((576, 2048), BF16),
            pltpu.VMEM((4, 512, 2048), BF16),
            pltpu.VMEM((4, 4, 2, 288, 128), F32),
            pltpu.VMEM((4, 2, 288, 128), F32),
            pltpu.VMEM((4, 2, 2, 288, 128), F32),
            pltpu.VMEM((3, 576, 128), F32),
            pltpu.VMEM((3, 128, 512), BF16),
            pltpu.VMEM((4, 4, 128, 512), BF16),
            pltpu.VMEM((256, 1152), BF16),
            pltpu.VMEM((4, 288, 2048), BF16),
            pltpu.VMEM((4, 4, 2, 72, 256), F32),
            pltpu.VMEM((4, 2, 72, 256), F32),
            pltpu.VMEM((4, 2, 2, 72, 256), F32),
            pltpu.VMEM((3, 72, 512), F32),
            pltpu.SemaphoreType.DMA((N_SEND,)),
            pltpu.SemaphoreType.DMA((N_COME,)),
            pltpu.SemaphoreType.DMA((7,)),
        ],
        compiler_params=pltpu.CompilerParams(
            collective_id=0, has_side_effects=True, vmem_limit_bytes=40 * 1024 * 1024
        ),
        name="weight_grads",
    )(*[pltpu.with_memory_space_constraint(v, pltpu.HBM) for v in flat])
    out_q, out_o = pl.pallas_call(
        store,
        out_shape=(
            jax.ShapeDtypeStruct((2304, 128), F32),
            jax.ShapeDtypeStruct((72, 2048), F32),
        ),
        in_specs=[vmem] * 2,
        out_specs=[hbm] * 2,
        scratch_shapes=[pltpu.SemaphoreType.DMA((5,))],
        compiler_params=pltpu.CompilerParams(vmem_limit_bytes=1024 * 1024),
        name="store",
    )(out_q, out_o)
    return out_q, out_o.T


def solution(mesh):
    in_specs = (
        P("col", "depth", "row"),
        P("row", "depth", "col"),
        P("col", "depth", "row"),
        P("row", "depth", "col"),
    )
    out_specs = (P("row", ("col", "depth")), P("row", ("col", "depth")))
    return jax.shard_map(
        per_device, mesh=mesh, in_specs=in_specs, out_specs=out_specs, check_vma=False
    )
```
